32 devices in a mesh: cells: 8 (over z, x), genes: 4 (over y, core).
Axes of the slice: x: 2, y: 2, z: 4, core: 2. Of those that a mesh axis runs over, the one named last changes fastest.
Arguments:
- counts: int32 [38912, 4000], P('cells', 'genes'), may hold values from 0 to 674, as said below
- sketch: bfloat16 [4000, 128], P('genes'), may hold values from -6 to 6
Outputs:
- basis: float32 [38912, 128], P('cells')
- loadings: float32 [4000, 128], P('genes')
The draws below stay inside these ranges and needn't reach their ends.
Inputs may be any that keep to these rules, and one draw needn't show every extreme that they name: `counts`: every cell and every gene has a positive total.
All inputs are finite; a program needn't handle non-finite values.
Results may differ from the reference program's by a relative error of at most 0.0051.
Values may be sent and summed in bfloat16 or wider, within the bound.
A program may use at most 128 MiB of HBM per device.

```python
import math
import jax
import jax.numpy as jnp
from jax import lax

CELL_DEV = 4864
GENES = 4000
RANK = 128
ITERS = 2
CELLS = 38912
N_CELLS = 8


def draw_counts(key, part):
    subkeys = jax.random.split(key, 4)
    row_ids = jnp.arange(CELLS, dtype=jnp.int32)[:, None]
    col_ids = jnp.arange(GENES, dtype=jnp.int32)[None, :]
    level_exp = jax.random.randint(subkeys[0], (1, GENES), 0, 2)
    gene_level = jnp.left_shift(jnp.int32(1), level_exp) * (12 * col_ids // GENES + 1)
    cell_level = jax.random.randint(subkeys[1], (CELLS, 1), 1, 4) * (6 * row_ids // CELLS + 2)
    ceiling = (gene_level * cell_level + 15) // 16
    background = jax.random.randint(subkeys[2], (CELLS, GENES), 0, ceiling + 1)
    marker = (col_ids == row_ids % GENES).astype(jnp.int32)
    rolled = jax.random.randint(subkeys[3], (CELLS, GENES), 0, 6400 * GENES)
    spikes = jnp.where(rolled < 400, 200 + rolled, 0)
    return (background + marker + spikes).astype(jnp.int32)


def block_scale(rng, extent, pieces, low, high):
    loudness = 1.0
    for position, shards_of in pieces:
        steps = jax.random.uniform(jax.random.fold_in(jax.random.fold_in(rng, 6), position), (shards_of,), jnp.float32, low / len(pieces), high / len(pieces))
        loudness = loudness * jnp.repeat(jnp.exp(steps), extent[position] // shards_of).reshape((-1,) + (1,) * (len(extent) - 1 - position))
    return loudness


def centred(key, extent, scale, most, cuts=(), kind=jnp.bfloat16):
    values = scale * jax.random.normal(key, extent, jnp.float32)
    if cuts:
        values = values * block_scale(key, extent, cuts, -0.22, 0.18)
    return jnp.clip(values, -most, most).astype(kind)


def setup_inputs(seed: int = 0) -> dict:
    key_list = jax.random.split(jax.random.key(seed), 3)
    return {
        "counts": draw_counts(jax.random.fold_in(key_list[2], 71), 0),
        "sketch": centred(key_list[1], (GENES, RANK), 1.0, 6.0, ((0, 4),)),
    }


def residual_block(block, cell_total, frac, limit):
    values = block.astype(jnp.float32)
    expected = cell_total[:, None] * frac[None, :]
    scaled = (values - expected) / jnp.sqrt(expected + 0.01 * expected * expected)
    return jnp.clip(scaled, -limit, limit).astype(jnp.bfloat16)

def self_gram(block):
    return lax.dot_general(block.astype(jnp.float32), block.astype(jnp.float32), (((0,), (0,)), ((), ())), precision=lax.Precision.HIGHEST, preferred_element_type=jnp.float32)

def whitening(gram, count):
    width = gram.shape[0]
    identity = jnp.eye(width, dtype=jnp.float32)
    shifted = gram + 1e-05 * jnp.trace(gram) / width * identity
    lower = jnp.linalg.cholesky(shifted)
    inverse = jax.scipy.linalg.solve_triangular(lower, identity, lower=True)
    return jnp.transpose(inverse) * math.sqrt(count)

def reference(counts, sketch):
    cell_total = lax.optimization_barrier(jnp.sum(counts, axis=1)).astype(jnp.float32)
    gene_total = lax.optimization_barrier(jnp.sum(counts, axis=0)).astype(jnp.float32)
    grand = jnp.sum(gene_total)
    frac = gene_total / grand
    limit = math.sqrt(float(CELLS))
    blocks = counts.reshape(N_CELLS, CELL_DEV, GENES)
    cell_blocks = cell_total.reshape(N_CELLS, CELL_DEV)
    gene_scale = math.sqrt(float(GENES)) / float(CELLS)
    omega = sketch
    basis = None
    loadings = None
    for sweep in range(ITERS):

        def sketch_block(operands, omega=omega):
            resid = residual_block(operands[0], operands[1], frac, limit)
            return jnp.dot(resid.astype(jnp.float32), omega.astype(jnp.float32), preferred_element_type=jnp.float32)
        sketched = lax.map(sketch_block, (blocks, cell_blocks)).reshape(CELLS, RANK)
        basis = jnp.dot(sketched, whitening(self_gram(sketched), float(CELLS)), precision=lax.Precision.HIGHEST)
        basis_blocks = basis.astype(jnp.bfloat16).reshape(N_CELLS, CELL_DEV, RANK)

        def add_block(total, operands):
            resid = residual_block(operands[0], operands[1], frac, limit)
            term = lax.dot_general(resid.astype(jnp.float32), operands[2].astype(jnp.float32), (((0,), (0,)), ((), ())), preferred_element_type=jnp.float32)
            return (total + term, None)
        start_total = jnp.zeros((GENES, RANK), jnp.float32)
        summed, _ = lax.scan(add_block, start_total, (blocks, cell_blocks, basis_blocks))
        loadings = summed * gene_scale
        if sweep < ITERS - 1:
            omega = loadings.astype(jnp.bfloat16)
    return (basis, loadings)
```

```python
import functools
import math

import jax
import jax.numpy as jnp
from jax import lax
from jax.experimental import pallas as pl
from jax.experimental.pallas import tpu as pltpu
from jax.sharding import PartitionSpec as P

ITERS = 2
CHUNK = 256
HALF = CHUNK // 2
BLOCK = 64
NEAR_LAG = 2
BASIS_LAG = 2
CODE = 32767.0
MIDDLE = 32768.0
MESH = pl.DeviceIdType.MESH


def ring_peers(axis, count):
    me = lax.axis_index(axis)
    return [{axis: lax.rem(me + step, count)} for step in range(1, count)]


def remote(src, dst, send_sem, recv_sem, peer):
    return pltpu.make_async_remote_copy(
        src_ref=src, dst_ref=dst, send_sem=send_sem, recv_sem=recv_sem, device_id=peer, device_id_type=MESH
    )


def encode(values):
    half = values.shape[0] // 2
    most = jnp.max(jnp.abs(values), axis=0, keepdims=True)
    inverse = jnp.where(most > 1e-30, CODE / most, 0.0)
    codes = (values * inverse + (MIDDLE + 0.5)).astype(jnp.int32)
    packed = codes[:half] | lax.shift_left(codes[half:], jnp.int32(16))
    return packed, most * (1.0 / CODE)


def decode(packed, unit):
    low = lax.bitwise_and(packed, jnp.int32(0xFFFF)).astype(jnp.float32)
    high = lax.shift_right_logical(packed, jnp.int32(16)).astype(jnp.float32)
    return jnp.concatenate([low - MIDDLE, high - MIDDLE], axis=0) * unit


def dot(left, right, left_dim, right_dim, precision=None):
    return lax.dot_general(
        left,
        right,
        (((left_dim,), (right_dim,)), ((), ())),
        precision=precision,
        preferred_element_type=jnp.float32,
    )


def split_terms(values):
    high = values.astype(jnp.bfloat16)
    return high, (values - high.astype(jnp.float32)).astype(jnp.bfloat16)


def whiten(gram, scale, out_ref, left, right):
    width = gram.shape[0]
    eye = lax.broadcasted_iota(jnp.int32, (width, width), 0) == lax.broadcasted_iota(jnp.int32, (width, width), 1)
    diagonal = jnp.where(eye, gram, 0.0)
    trace = jnp.sum(jnp.sum(diagonal, axis=1, keepdims=True), axis=0, keepdims=True)
    left[...] = gram + jnp.where(eye, 1e-05 * trace / width, 0.0)
    right[...] = jnp.where(eye, 1.0, 0.0)
    place = lax.broadcasted_iota(jnp.int32, (8, width), 0)

    def panel(step, carry):
        rows_left, rows_right = left[:8, :], right[:8, :]
        columns = [jnp.broadcast_to(rows_left[:, i : i + 1], (8, width)) for i in range(8)]
        done_left = jnp.zeros((8, width), jnp.float32)
        done_right = jnp.zeros((8, width), jnp.float32)
        for i in range(8):
            inverse = lax.rsqrt(columns[i][i : i + 1, :])
            top_left, top_right = rows_left[i : i + 1, :] * inverse, rows_right[i : i + 1, :] * inverse
            done_left = jnp.where(place == i, top_left, done_left)
            done_right = jnp.where(place == i, top_right, done_right)
            if i < 7:
                factor = jnp.where(place > i, columns[i] * inverse, 0.0)
                rows_left = rows_left - factor * top_left
                rows_right = rows_right - factor * top_right
                for j in range(i + 1, 8):
                    columns[j] = columns[j] - factor * (columns[j][i : i + 1, :] * inverse)
        out_ref[pl.ds(pl.multiple_of(step * 8, 8), 8), :] = done_right * scale
        new_left = pltpu.roll(left[...] - dot(done_left, done_left, 0, 0, lax.Precision.HIGHEST), width - 8, 1)
        new_right = right[...] - dot(done_left, done_right, 0, 0, lax.Precision.HIGHEST)
        left[: width - 8, :] = new_left[8:, :]
        right[: width - 8, :] = new_right[8:, :]
        left[width - 8 :, :] = jnp.zeros((8, width), jnp.float32)
        right[width - 8 :, :] = jnp.zeros((8, width), jnp.float32)
        return carry

    lax.fori_loop(0, width // 8, panel, 0)


def loop(count, body):
    lax.fori_loop(0, count, lambda i, carry: (body(i), carry)[1], 0)


def body(
    n,
    m,
    gene_dev,
    limit,
    gene_scale,
    counts_ref,
    sketch_ref,
    basis_ref,
    load_ref,
    counts,
    resid,
    gene_acc,
    frac,
    omega,
    part,
    near,
    codes,
    units,
    terms,
    product,
    gram_acc,
    gene_all,
    cell_all,
    grand_all,
    gram_all,
    gram_rows,
    gram_part,
    load_part,
    load_part_unit,
    load_all,
    load_unit,
    load_sum,
    load_sum_unit,
    left,
    right,
    white,
    in_sem,
    gene_sem,
    cell_sem,
    grand_sem,
    near_sem,
    code_sem,
    unit_sem,
    term_sem,
    gram_sem,
    rows_sem,
    piece_sem,
    piece_unit_sem,
    all_sem,
    all_unit_sem,
):
    f32, bf16 = jnp.float32, jnp.bfloat16
    chunks, rows8, _ = counts.shape
    padded = resid.shape[1]
    width = left.shape[0]
    gene_rows = padded // 128
    cells_me, genes_me = lax.axis_index("cells"), lax.axis_index("genes")
    y_count = m // 2
    core, row = lax.rem(genes_me, 2), lax.div(genes_me, 2)
    partner = {"genes": row * 2 + 1 - core}
    y_peers = [{"genes": lax.rem(row + step, y_count) * 2 + core} for step in range(1, y_count)]
    cell_peers = ring_peers("cells", n)
    gene_peers = ring_peers("genes", m)

    def fetch(i):
        start = pl.multiple_of(i * CHUNK, CHUNK)
        return pltpu.make_async_copy(counts_ref.at[:, pl.ds(start, CHUNK)], counts.at[i], in_sem.at[i])

    loop(chunks, lambda i: fetch(i).start())
    barrier = pltpu.get_barrier_semaphore()
    for peer in cell_peers + gene_peers:
        pl.semaphore_signal(barrier, inc=1, device_id=peer, device_id_type=MESH)
    gene_acc[...] = jnp.zeros(gene_acc.shape, jnp.int32)
    omega[...] = jnp.zeros(omega.shape, bf16)
    omega[:gene_dev, :] = sketch_ref[...]
    step_rows = max(k for k in range(8, 65, 8) if rows8 % k == 0)

    def total_chunk(i):
        fetch(i).wait()

        def add(k, total):
            start = pl.ds(pl.multiple_of(k * step_rows, 8), step_rows)
            block = counts[i, start, :]
            gene_acc[start, :] += block[:, :HALF] + block[:, HALF:]
            for r in range(0, step_rows, 8):
                total = total + block[r : r + 8, :]
            return total

        total = lax.fori_loop(0, rows8 // step_rows, add, jnp.zeros((8, CHUNK), jnp.int32))
        cell_all[genes_me, i] = jnp.sum(total, axis=0, keepdims=True).astype(f32)

    loop(chunks, total_chunk)
    for b in range(gene_rows):
        across = gene_acc[128 * b : 128 * (b + 1), :].astype(f32).T
        gene_all[cells_me, b] = jnp.sum(across, axis=0, keepdims=True)
    pl.semaphore_wait(barrier, len(cell_peers) + len(gene_peers))

    def share(buffer, place, sem, peers):
        copies = [
            remote(buffer.at[place], buffer.at[place], sem.at[0, i], sem.at[1, i], peer) for i, peer in enumerate(peers)
        ]
        for copy in copies:
            copy.start()
        return copies

    pending = []
    gene_copies = share(gene_all, cells_me, gene_sem, cell_peers)
    cell_copies = share(cell_all, genes_me, cell_sem, gene_peers)
    for copy in gene_copies:
        copy.wait_recv()
    gene_total = gene_all[0]
    for s in range(1, n):
        gene_total = gene_total + gene_all[s]
    grand = jnp.sum(jnp.sum(gene_total, axis=0), axis=1, keepdims=True)
    grand_all[genes_me] = jnp.broadcast_to(grand, (8, 128))
    grand_copies = share(grand_all, genes_me, grand_sem, gene_peers)
    for copy in grand_copies:
        copy.wait_recv()
    grand = grand_all[0]
    for s in range(1, m):
        grand = grand + grand_all[s]
    for b in range(gene_rows):
        share_row = jnp.where(gene_total[b] > 0.0, gene_total[b] / grand[:1], 1.0)
        frac[128 * b : 128 * (b + 1), :] = jnp.broadcast_to(share_row, (128, 128)).T
    for copy in cell_copies:
        copy.wait_recv()
    pending += gene_copies + cell_copies + grand_copies

    def residual(i):
        cell_total = cell_all[0, i]
        for s in range(1, m):
            cell_total = cell_total + cell_all[s, i]

        def block(start, real):
            values = counts[i, pl.ds(start, real), :].astype(f32)
            share_of = frac[pl.ds(start, real), :]
            expected = jnp.concatenate([share_of, share_of], axis=1) * cell_total
            scaled = (values - expected) * lax.rsqrt(expected + 0.01 * expected * expected)
            return jnp.clip(scaled, -limit, limit).astype(bf16)

        def full(k):
            start = pl.multiple_of(k * BLOCK, BLOCK)
            resid[i, pl.ds(start, BLOCK), :] = block(start, BLOCK)

        loop(rows8 // BLOCK, full)
        done = rows8 // BLOCK * BLOCK
        if rows8 > done:
            last = block(done, rows8 - done)
            resid[i, done : done + BLOCK, :] = jnp.concatenate(
                [last, jnp.zeros((done + BLOCK - rows8, CHUNK), bf16)], axis=0
            )
            done += BLOCK
        if padded > done:
            resid[i, done:, :] = jnp.zeros((padded - done, CHUNK), bf16)

    for sweep in range(ITERS):

        def near_copy(i):
            return remote(
                part.at[sweep, i, 1 - core],
                near.at[sweep, i],
                near_sem.at[sweep, 0, i],
                near_sem.at[sweep, 1, i],
                partner,
            )

        def code_copies(i):
            pairs = []
            for s, peer in enumerate(y_peers):
                for buffer, sem in ((codes, code_sem), (units, unit_sem)):
                    here = buffer.at[sweep, row, i]
                    pairs.append(remote(here, here, sem.at[sweep, 0, s, i], sem.at[sweep, 1, s, i], peer))
            return pairs

        def term_copy(i):
            here = terms.at[sweep, i, core]
            return remote(here, here, term_sem.at[sweep, 0, i], term_sem.at[sweep, 1, i], partner)

        def first(i):
            @pl.when(i < chunks)
            def _():
                if sweep == 0:
                    residual(i)
                rows = dot(resid[i], omega[...], 0, 0)
                part[sweep, i, 0] = rows[:HALF]
                part[sweep, i, 1] = rows[HALF:]
                near_copy(i).start()

            @pl.when(i >= NEAR_LAG)
            def _():
                j = i - NEAR_LAG
                near_copy(j).wait_recv()
                packed, unit = encode(part[sweep, j, core] + near[sweep, j])
                codes[sweep, row, j] = packed
                units[sweep, row, j] = unit
                for copy in code_copies(j):
                    copy.start()

        loop(chunks + NEAR_LAG, first)
        product[...] = jnp.zeros(product.shape, f32)
        gram_acc[...] = jnp.zeros(gram_acc.shape, f32)

        def second(i):
            @pl.when(i < chunks)
            def _():
                for copy in code_copies(i):
                    copy.wait_recv()
                total = decode(codes[sweep, 0, i], units[sweep, 0, i])
                for s in range(1, y_count):
                    total = total + decode(codes[sweep, s, i], units[sweep, s, i])
                high, low = split_terms(total)
                terms[sweep, i, core] = jnp.concatenate([high, low], axis=1)
                term_copy(i).start()

            @pl.when(i >= BASIS_LAG)
            def _():
                j = i - BASIS_LAG
                term_copy(j).wait_recv()
                both = terms[sweep, j].reshape(CHUNK, 2 * width)
                gram_acc[...] += dot(both, both, 0, 0)
                product[...] += dot(resid[j], both, 1, 0)

        loop(chunks + BASIS_LAG, second)

        gram = gram_acc[:width, :width] + gram_acc[:width, width:] + (gram_acc[width:, :width] + gram_acc[width:, width:])
        strip = width // m
        for g in range(m):
            gram_part[g] = gram[strip * g : strip * (g + 1)]
        gram_all[sweep, cells_me] = gram_part[genes_me]
        gram_copies = share(gram_all.at[sweep], cells_me, gram_sem.at[sweep], cell_peers)
        piece = padded // n
        for p in range(n):
            mine = product[piece * p : piece * (p + 1), :width] + product[piece * p : piece * (p + 1), width:]
            packed, unit = encode(mine)
            load_part[sweep, p] = packed
            load_part_unit[sweep, p] = unit
        piece_copies = []
        for s, peer in enumerate(cell_peers):
            for src, dst, sem in (
                (load_part, load_all, piece_sem),
                (load_part_unit, load_unit, piece_unit_sem),
            ):
                copy = remote(
                    src.at[sweep, peer["cells"]], dst.at[sweep, cells_me], sem.at[sweep, 0, s], sem.at[sweep, 1, s], peer
                )
                copy.start()
                piece_copies.append(copy)
        load_all[sweep, cells_me] = load_part[sweep, cells_me]
        load_unit[sweep, cells_me] = load_part_unit[sweep, cells_me]
        for copy in gram_copies:
            copy.wait_recv()
        total = gram_all[sweep, 0]
        for s in range(1, n):
            total = total + gram_all[sweep, s]
        gram_rows[sweep, genes_me] = total
        rows_copies = share(gram_rows.at[sweep], genes_me, rows_sem.at[sweep], gene_peers)
        for copy in piece_copies:
            copy.wait_recv()
        total = decode(load_all[sweep, 0], load_unit[sweep, 0])
        for s in range(1, n):
            total = total + decode(load_all[sweep, s], load_unit[sweep, s])
        packed, unit = encode(total)
        load_sum[sweep, cells_me] = packed
        load_sum_unit[sweep, cells_me] = unit
        all_copies = share(load_sum.at[sweep], cells_me, all_sem.at[sweep], cell_peers)
        all_copies += share(load_sum_unit.at[sweep], cells_me, all_unit_sem.at[sweep], cell_peers)
        for copy in rows_copies:
            copy.wait_recv()
        whiten(gram_rows[sweep].reshape(width, width), math.sqrt(chunks * CHUNK * n), white, left, right)
        last = sweep == ITERS - 1
        if last:
            high, low = split_terms(white[...].T)
            wide = jnp.concatenate([high, low], axis=1)
            wide = jnp.concatenate([wide, wide], axis=0)

            def write(i):
                rows = dot(terms[sweep, i].reshape(CHUNK, 2 * width), wide, 1, 0)
                start = pl.multiple_of(i * CHUNK, CHUNK)
                basis_ref[pl.ds(start, CHUNK), :] = rows[:, :width] + rows[:, width:]

            loop(chunks, write)
        for copy in all_copies:
            copy.wait_recv()
        scaled_white = white[...] * gene_scale
        for p in range(n):
            loads = dot(decode(load_sum[sweep, p], load_sum_unit[sweep, p]), scaled_white, 1, 1, lax.Precision.HIGHEST)
            start, stop = piece * p, min(piece * (p + 1), gene_dev)
            if last and stop > start:
                load_ref[start:stop, :] = loads[: stop - start]
            elif not last:
                omega[start : piece * (p + 1), :] = loads.astype(bf16)
        for copy in gram_copies + piece_copies + rows_copies + all_copies:
            copy.wait_send()

        def drain(i):
            near_copy(i).wait_send()
            for copy in code_copies(i):
                copy.wait_send()
            term_copy(i).wait_send()

        loop(chunks, drain)
    for copy in pending:
        copy.wait_send()


def shards(counts, sketch):
    cell_dev, gene_dev = counts.shape
    n, m = lax.axis_size("cells"), lax.axis_size("genes")
    width = sketch.shape[1]
    rows8 = -(-gene_dev // 8) * 8
    unit = max(16 * n, 128)
    padded = -(-gene_dev // unit) * unit
    chunks = cell_dev // CHUNK
    assert chunks * CHUNK == cell_dev and m % 2 == 0 and width % (8 * m) == 0
    table = counts.T
    if rows8 > gene_dev:
        table = jnp.pad(table, ((0, rows8 - gene_dev), (0, 0)))
    cell_count = float(cell_dev * n)
    gene_scale = math.sqrt(float(gene_dev * m)) / cell_count
    f32, bf16, i32 = jnp.float32, jnp.bfloat16, jnp.int32
    y_count = m // 2
    piece = padded // n
    vmem = pltpu.VMEM
    dma = pltpu.SemaphoreType.DMA
    scratch = [
        vmem((chunks, rows8, CHUNK), i32),
        vmem((chunks, padded, CHUNK), bf16),
        vmem((padded, 128), i32),
        vmem((padded, 128), f32),
        vmem((padded, width), bf16),
        vmem((ITERS, chunks, 2, HALF, width), f32),
        vmem((ITERS, chunks, HALF, width), f32),
        vmem((ITERS, y_count, chunks, HALF // 2, width), i32),
        vmem((ITERS, y_count, chunks, 1, width), f32),
        vmem((ITERS, chunks, 2, HALF, 2 * width), bf16),
        vmem((padded, 2 * width), f32),
        vmem((2 * width, 2 * width), f32),
        vmem((n, padded // 128, 1, 128), f32),
        vmem((m, chunks, 1, CHUNK), f32),
        vmem((m, 8, 128), f32),
        vmem((ITERS, n, width // m, width), f32),
        vmem((ITERS, m, width // m, width), f32),
        vmem((m, width // m, width), f32),
        vmem((ITERS, n, piece // 2, width), i32),
        vmem((ITERS, n, 1, width), f32),
        vmem((ITERS, n, piece // 2, width), i32),
        vmem((ITERS, n, 1, width), f32),
        vmem((ITERS, n, piece // 2, width), i32),
        vmem((ITERS, n, 1, width), f32),
        vmem((width, width), f32),
        vmem((width, width), f32),
        vmem((width, width), f32),
        dma((chunks,)),
        dma((2, n - 1)),
        dma((2, m - 1)),
        dma((2, m - 1)),
        dma((ITERS, 2, chunks)),
        dma((ITERS, 2, max(y_count - 1, 1), chunks)),
        dma((ITERS, 2, max(y_count - 1, 1), chunks)),
        dma((ITERS, 2, chunks)),
        dma((ITERS, 2, n - 1)),
        dma((ITERS, 2, m - 1)),
        dma((ITERS, 2, n - 1)),
        dma((ITERS, 2, n - 1)),
        dma((ITERS, 2, n - 1)),
        dma((ITERS, 2, n - 1)),
    ]
    basis, loadings = pl.pallas_call(
        functools.partial(body, n, m, gene_dev, math.sqrt(cell_count), gene_scale),
        out_shape=[jax.ShapeDtypeStruct((cell_dev, width), f32), jax.ShapeDtypeStruct((gene_dev, width), f32)],
        in_specs=[pl.BlockSpec(memory_space=pl.ANY), pl.BlockSpec(memory_space=pltpu.VMEM)],
        out_specs=[pl.BlockSpec(memory_space=pltpu.VMEM)] * 2,
        scratch_shapes=scratch,
        compiler_params=pltpu.CompilerParams(
            collective_id=0, has_side_effects=True, vmem_limit_bytes=58 * 1024 * 1024
        ),
    )(table, sketch)
    return basis, loadings


def solution(mesh):
    return jax.shard_map(
        shards,
        mesh=mesh,
        in_specs=(P("cells", "genes"), P("genes", None)),
        out_specs=(P("cells", None), P("genes", None)),
        check_vma=False,
    )
```

```python
import functools
import math

import jax
import jax.numpy as jnp
from jax import lax
from jax.experimental import pallas as pl
from jax.experimental.pallas import tpu as pltpu
from jax.sharding import PartitionSpec as P

ITERS = 2
CHUNK = 256
HALF = CHUNK // 2
BLOCK = 64
DEPTH = 256
NEAR_LAG = 4
EARLY_PANELS = 4
BASIS_LAG = 4
CODE = 32767.0
MIDDLE = 32768.0
MESH = pl.DeviceIdType.MESH


def ring_peers(axis, count):
    me = lax.axis_index(axis)
    return [{axis: lax.rem(me + step, count)} for step in range(1, count)]


def remote(src, dst, send_sem, recv_sem, peer):
    return pltpu.make_async_remote_copy(
        src_ref=src, dst_ref=dst, send_sem=send_sem, recv_sem=recv_sem, device_id=peer, device_id_type=MESH
    )


def encode(values):
    half = values.shape[0] // 2
    most = jnp.max(jnp.abs(values), axis=0, keepdims=True)
    inverse = jnp.where(most > 1e-30, CODE / most, 0.0)
    codes = (values * inverse + (MIDDLE + 0.5)).astype(jnp.int32)
    packed = codes[:half] | lax.shift_left(codes[half:], jnp.int32(16))
    return packed, most * (1.0 / CODE)


def decode(packed, unit):
    low = lax.bitwise_and(packed, jnp.int32(0xFFFF)).astype(jnp.float32)
    high = lax.shift_right_logical(packed, jnp.int32(16)).astype(jnp.float32)
    return jnp.concatenate([low - MIDDLE, high - MIDDLE], axis=0) * unit


def dot(left, right, left_dim, right_dim, precision=None):
    return lax.dot_general(
        left,
        right,
        (((left_dim,), (right_dim,)), ((), ())),
        precision=precision,
        preferred_element_type=jnp.float32,
    )


def split_terms(values):
    high = values.astype(jnp.bfloat16)
    return high, (values - high.astype(jnp.float32)).astype(jnp.bfloat16)


def whiten_start(gram, left, right):
    width = gram.shape[0]
    eye = lax.broadcasted_iota(jnp.int32, (width, width), 0) == lax.broadcasted_iota(jnp.int32, (width, width), 1)
    diagonal = jnp.where(eye, gram, 0.0)
    trace = jnp.sum(jnp.sum(diagonal, axis=1, keepdims=True), axis=0, keepdims=True)
    left[...] = gram + jnp.where(eye, 1e-05 * trace / width, 0.0)
    right[...] = jnp.where(eye, 1.0, 0.0)


def whiten_panels(start, stop, scale, out_ref, left, right):
    width = left.shape[0]
    place = lax.broadcasted_iota(jnp.int32, (8, width), 0)

    def panel(step, carry):
        rows_left, rows_right = left[:8, :], right[:8, :]
        columns = [jnp.broadcast_to(rows_left[:, i : i + 1], (8, width)) for i in range(8)]
        done_left = jnp.zeros((8, width), jnp.float32)
        done_right = jnp.zeros((8, width), jnp.float32)
        for i in range(8):
            inverse = lax.rsqrt(columns[i][i : i + 1, :])
            top_left, top_right = rows_left[i : i + 1, :] * inverse, rows_right[i : i + 1, :] * inverse
            done_left = jnp.where(place == i, top_left, done_left)
            done_right = jnp.where(place == i, top_right, done_right)
            if i < 7:
                factor = jnp.where(place > i, columns[i] * inverse, 0.0)
                rows_left = rows_left - factor * top_left
                rows_right = rows_right - factor * top_right
                for j in range(i + 1, 8):
                    columns[j] = columns[j] - factor * (columns[j][i : i + 1, :] * inverse)
        out_ref[pl.ds(pl.multiple_of(step * 8, 8), 8), :] = done_right * scale
        new_left = pltpu.roll(left[...] - dot(done_left, done_left, 0, 0, lax.Precision.HIGHEST), width - 8, 1)
        new_right = right[...] - dot(done_left, done_right, 0, 0, lax.Precision.HIGHEST)
        left[: width - 8, :] = new_left[8:, :]
        right[: width - 8, :] = new_right[8:, :]
        left[width - 8 :, :] = jnp.zeros((8, width), jnp.float32)
        right[width - 8 :, :] = jnp.zeros((8, width), jnp.float32)
        return carry

    lax.fori_loop(start, stop, panel, 0)


def loop(count, body):
    lax.fori_loop(0, count, lambda i, carry: (body(i), carry)[1], 0)


def staged(count, lag, step):
    lag = min(lag, count)
    loop(lag, lambda i: step(i, True, False))
    lax.fori_loop(lag, count, lambda i, carry: (step(i, True, True), carry)[1], 0)
    lax.fori_loop(count, count + lag, lambda i, carry: (step(i, False, True), carry)[1], 0)


def body(
    n,
    m,
    gene_dev,
    limit,
    gene_scale,
    counts_ref,
    sketch_ref,
    basis_ref,
    load_ref,
    counts,
    resid,
    gene_acc,
    frac,
    omega,
    part,
    near,
    codes,
    units,
    terms,
    product,
    gram_acc,
    gene_all,
    cell_all,
    grand_all,
    gram_all,
    gram_rows,
    gram_part,
    load_part,
    load_part_unit,
    load_all,
    load_unit,
    load_sum,
    load_sum_unit,
    left,
    right,
    white,
    in_sem,
    gene_sem,
    cell_sem,
    grand_sem,
    near_sem,
    code_sem,
    unit_sem,
    term_sem,
    gram_sem,
    rows_sem,
    piece_sem,
    piece_unit_sem,
    all_sem,
    all_unit_sem,
):
    f32, bf16 = jnp.float32, jnp.bfloat16
    chunks, rows8, _ = counts.shape
    padded = resid.shape[1]
    width = left.shape[0]
    gene_rows = padded // 128
    cells_me, genes_me = lax.axis_index("cells"), lax.axis_index("genes")
    y_count = m // 2
    core, row = lax.rem(genes_me, 2), lax.div(genes_me, 2)
    partner = {"genes": row * 2 + 1 - core}
    y_peers = [{"genes": lax.rem(row + step, y_count) * 2 + core} for step in range(1, y_count)]
    cell_peers = ring_peers("cells", n)
    gene_peers = ring_peers("genes", m)

    def fetch(i):
        start = pl.multiple_of(i * CHUNK, CHUNK)
        return pltpu.make_async_copy(counts_ref.at[:, pl.ds(start, CHUNK)], counts.at[i], in_sem.at[i])

    loop(chunks, lambda i: fetch(i).start())
    sketch_copy = pltpu.make_async_copy(sketch_ref, omega.at[pl.ds(0, rows8)], in_sem.at[chunks])
    sketch_copy.start()
    barrier = pltpu.get_barrier_semaphore()

    def other(s):
        return {"cells": lax.rem(cells_me + lax.div(s, m), n), "genes": lax.rem(genes_me + lax.rem(s, m), m)}

    def greet(s):
        pl.semaphore_signal(barrier, inc=1, device_id=other(s + 1), device_id_type=MESH)

    loop(n * m - 1, greet)
    gene_acc[...] = jnp.zeros(gene_acc.shape, jnp.int32)
    if padded > rows8:
        omega[rows8:, :] = jnp.zeros((padded - rows8, width), bf16)
    step_rows = max(k for k in range(8, 65, 8) if rows8 % k == 0)

    def total_chunk(i):
        fetch(i).wait()

        def add(k, total):
            start = pl.ds(pl.multiple_of(k * step_rows, 8), step_rows)
            block = counts[i, start, :]
            gene_acc[start, :] += block[:, :HALF] + block[:, HALF:]
            for r in range(0, step_rows, 8):
                total = total + block[r : r + 8, :]
            return total

        total = lax.fori_loop(0, rows8 // step_rows, add, jnp.zeros((8, CHUNK), jnp.int32))
        cell_all[genes_me, i] = jnp.sum(total, axis=0, keepdims=True).astype(f32)

    with jax.named_scope("stream"):
        loop(chunks, total_chunk)
    for b in range(gene_rows):
        across = gene_acc[128 * b : 128 * (b + 1), :].astype(f32).T
        gene_row = jnp.sum(across, axis=0, keepdims=True)
        gene_all[cells_me, b] = gene_row
        grand = gene_row if b == 0 else grand + gene_row
    grand_all[cells_me * m + genes_me] = jnp.broadcast_to(jnp.sum(grand, axis=1, keepdims=True), (1, 128))
    with jax.named_scope("barrier"):
        pl.semaphore_wait(barrier, n * m - 1)

    def send_all(src, dst, sem, peers):
        for s, peer in enumerate(peers):
            remote(src(peer), dst, sem.at[0], sem.at[1], peer).start()

    def share(buffer, place, sem, peers):
        send_all(lambda peer: buffer.at[place], buffer.at[place], sem, peers)
        everything = buffer.at[pl.ds(0, len(peers))]
        return remote(everything, everything, sem.at[0], sem.at[1], peers[0])

    gene_copies = share(gene_all, cells_me, gene_sem, cell_peers)
    cell_copies = share(cell_all, genes_me, cell_sem, gene_peers)
    me = cells_me * m + genes_me

    def grand_start(s):
        here = grand_all.at[me]
        remote(here, here, grand_sem.at[0], grand_sem.at[1], other(s + 1)).start()

    loop(n * m - 1, grand_start)
    everything = grand_all.at[pl.ds(0, n * m - 1)]
    grand_copies = remote(everything, everything, grand_sem.at[0], grand_sem.at[1], other(1))
    with jax.named_scope("wait_gene"):
        gene_copies.wait_recv()
    gene_total = gene_all[0]
    for s in range(1, n):
        gene_total = gene_total + gene_all[s]
    with jax.named_scope("wait_grand"):
        grand_copies.wait_recv()
    grand = jnp.sum(grand_all[...], axis=0)
    for b in range(gene_rows):
        share_row = jnp.where(gene_total[b] > 0.0, gene_total[b] / grand, 1.0)
        frac[128 * b : 128 * (b + 1), :] = jnp.broadcast_to(share_row, (128, 128)).T
    with jax.named_scope("wait_cell"):
        cell_copies.wait_recv()

    def residual(i):
        cell_total = cell_all[0, i]
        for s in range(1, m):
            cell_total = cell_total + cell_all[s, i]
        sums = None
        for start in range(0, padded, DEPTH):
            stop = min(start + DEPTH, padded)
            blocks = []
            for k in range(start, min(stop, rows8), BLOCK):
                real = min(k + BLOCK, stop, rows8) - k
                share_of = frac[k : k + real, :]
                expected = jnp.concatenate([share_of, share_of], axis=1) * cell_total
                scaled = (counts[i, k : k + real, :].astype(f32) - expected) * lax.rsqrt(
                    expected + 0.01 * expected * expected
                )
                blocks.append(jnp.clip(scaled, -limit, limit))
            if stop > rows8:
                blocks.append(jnp.zeros((stop - max(start, rows8), CHUNK), f32))
            values = jnp.concatenate(blocks, axis=0).astype(bf16)
            resid[i, start:stop, :] = values
            term = dot(values, omega[start:stop, :], 0, 0)
            sums = term if sums is None else sums + term
        return sums

    sketch_copy.wait()
    for sweep in range(ITERS):

        def near_copy(i):
            return remote(part.at[i, 1 - core], near.at[sweep, i], near_sem.at[chunks], near_sem.at[i], partner)

        def code_start(i):
            for peer in y_peers:
                for buffer, sem in ((codes, code_sem), (units, unit_sem)):
                    here = buffer.at[sweep, row, i]
                    remote(here, here, sem.at[chunks], sem.at[i], peer).start()

        def code_wait(i):
            for buffer, sem in ((codes, code_sem), (units, unit_sem)):
                here = buffer.at[sweep, pl.ds(0, y_count - 1), i]
                remote(here, here, sem.at[chunks], sem.at[i], y_peers[0]).wait_recv()

        def term_copy(i):
            here = terms.at[sweep, i, core]
            return remote(here, here, term_sem.at[chunks], term_sem.at[i], partner)

        def first(i, sketch, code):
            j = i - NEAR_LAG
            if code:
                near_copy(j).wait_recv()
                packed, unit = encode(part[j, core] + near[sweep, j])
                codes[sweep, row, j] = packed
                units[sweep, row, j] = unit
            if sketch:
                rows = residual(i) if sweep == 0 else dot(resid[i], omega[...], 0, 0)
                part[i, 0] = rows[:HALF]
                part[i, 1] = rows[HALF:]
                near_copy(i).start()
            if code:
                code_start(j)

        def second(i, decoding, multiply):
            j = i - BASIS_LAG
            if decoding:
                code_wait(i)
            if multiply:
                term_copy(j).wait_recv()
                both = terms[sweep, j].reshape(CHUNK, 2 * width)
                gram_acc[...] += dot(both, both, 0, 0)
                product[...] += dot(resid[j], both, 1, 0)
            if decoding:
                total = decode(codes[sweep, 0, i], units[sweep, 0, i])
                for s in range(1, y_count):
                    total = total + decode(codes[sweep, s, i], units[sweep, s, i])
                high, low = split_terms(total)
                terms[sweep, i, core] = jnp.concatenate([high, low], axis=1)
                term_copy(i).start()

        with jax.named_scope(f"first{sweep}"):
            staged(chunks, NEAR_LAG, first)
        product[...] = jnp.zeros(product.shape, f32)
        gram_acc[...] = jnp.zeros(gram_acc.shape, f32)
        with jax.named_scope(f"second{sweep}"):
            staged(chunks, BASIS_LAG, second)

        gram = gram_acc[:width, :width] + gram_acc[:width, width:] + (gram_acc[width:, :width] + gram_acc[width:, width:])
        strip = width // m
        for g in range(m):
            gram_part[g] = gram[strip * g : strip * (g + 1)]
        gram_all[sweep, cells_me] = gram_part[genes_me]
        gram_copies = share(gram_all.at[sweep], cells_me, gram_sem, cell_peers)
        piece = padded // n
        for p in range(n):
            mine = product[piece * p : piece * (p + 1), :width] + product[piece * p : piece * (p + 1), width:]
            packed, unit = encode(mine)
            load_part[sweep, p] = packed
            load_part_unit[sweep, p] = unit
        piece_copies = []
        for src, dst, sem in ((load_part, load_all, piece_sem), (load_part_unit, load_unit, piece_unit_sem)):
            send_all(lambda peer: src.at[sweep, peer["cells"]], dst.at[sweep, cells_me], sem, cell_peers)
            most = pl.ds(0, n - 1)
            piece_copies.append(
                remote(src.at[sweep, most], dst.at[sweep, most], sem.at[0], sem.at[1], cell_peers[0])
            )
        load_all[sweep, cells_me] = load_part[sweep, cells_me]
        load_unit[sweep, cells_me] = load_part_unit[sweep, cells_me]
        with jax.named_scope(f"wait_gram{sweep}"):
            gram_copies.wait_recv()
        total = gram_all[sweep, 0]
        for s in range(1, n):
            total = total + gram_all[sweep, s]
        gram_rows[sweep, genes_me] = total
        rows_copies = share(gram_rows.at[sweep], genes_me, rows_sem, gene_peers)
        with jax.named_scope(f"wait_rows{sweep}"):
            rows_copies.wait_recv()
        panels = width // 8
        early = min(EARLY_PANELS, panels)
        scale = math.sqrt(chunks * CHUNK * n)
        with jax.named_scope(f"whiten{sweep}"):
            whiten_start(gram_rows[sweep].reshape(width, width), left, right)
            whiten_panels(0, early, scale, white, left, right)
        with jax.named_scope(f"wait_piece{sweep}"):
            for copy in piece_copies:
                copy.wait_recv()
        total = decode(load_all[sweep, 0], load_unit[sweep, 0])
        for s in range(1, n):
            total = total + decode(load_all[sweep, s], load_unit[sweep, s])
        packed, unit = encode(total)
        load_sum[sweep, cells_me] = packed
        load_sum_unit[sweep, cells_me] = unit
        all_copies = share(load_sum.at[sweep], cells_me, all_sem, cell_peers)
        all_unit_copies = share(load_sum_unit.at[sweep], cells_me, all_unit_sem, cell_peers)
        with jax.named_scope(f"whiten{sweep}"):
            whiten_panels(early, panels, scale, white, left, right)
        last = sweep == ITERS - 1
        if last:
            high, low = split_terms(white[...].T)
            wide = jnp.concatenate([high, low], axis=1)
            wide = jnp.concatenate([wide, wide], axis=0)

            def write(i):
                rows = dot(terms[sweep, i].reshape(CHUNK, 2 * width), wide, 1, 0)
                start = pl.multiple_of(i * CHUNK, CHUNK)
                basis_ref[pl.ds(start, CHUNK), :] = rows[:, :width] + rows[:, width:]

            with jax.named_scope("write"):
                lax.fori_loop(0, chunks, lambda i, carry: (write(i), carry)[1], 0, unroll=True)
        with jax.named_scope(f"wait_all{sweep}"):
            all_copies.wait_recv()
            all_unit_copies.wait_recv()
        scaled_white = white[...] * gene_scale
        for p in range(n):
            loads = dot(decode(load_sum[sweep, p], load_sum_unit[sweep, p]), scaled_white, 1, 1, lax.Precision.HIGHEST)
            start, stop = piece * p, min(piece * (p + 1), gene_dev)
            if last and stop > start:
                load_ref[start:stop, :] = loads[: stop - start]
            elif not last:
                omega[start : piece * (p + 1), :] = loads.astype(bf16)
        for copies in [gram_copies, rows_copies, all_copies, all_unit_copies] + piece_copies:
            copies.wait_send()
        near_all, term_all = near.at[sweep], terms.at[sweep, pl.ds(0, chunks), core]
        remote(near_all, near_all, near_sem.at[chunks], near_sem.at[0], partner).wait_send()
        remote(term_all, term_all, term_sem.at[chunks], term_sem.at[0], partner).wait_send()
        for buffer, sem in ((codes, code_sem), (units, unit_sem)):
            here = buffer.at[sweep, pl.ds(0, y_count - 1)]
            remote(here, here, sem.at[chunks], sem.at[0], y_peers[0]).wait_send()
    for copies in (gene_copies, cell_copies, grand_copies):
        copies.wait_send()


def shards(counts, sketch):
    cell_dev, gene_dev = counts.shape
    n, m = lax.axis_size("cells"), lax.axis_size("genes")
    width = sketch.shape[1]
    rows8 = -(-gene_dev // 8) * 8
    unit = max(16 * n, 128)
    padded = -(-gene_dev // unit) * unit
    chunks = cell_dev // CHUNK
    assert chunks * CHUNK == cell_dev and m % 2 == 0 and width % (8 * m) == 0
    table = counts.T
    if rows8 > gene_dev:
        table = jnp.pad(table, ((0, rows8 - gene_dev), (0, 0)))
        sketch = jnp.pad(sketch, ((0, rows8 - gene_dev), (0, 0)))
    cell_count = float(cell_dev * n)
    gene_scale = math.sqrt(float(gene_dev * m)) / cell_count
    f32, bf16, i32 = jnp.float32, jnp.bfloat16, jnp.int32
    y_count = m // 2
    piece = padded // n
    vmem = pltpu.VMEM
    dma = pltpu.SemaphoreType.DMA
    scratch = [
        vmem((chunks, rows8, CHUNK), i32),
        vmem((chunks, padded, CHUNK), bf16),
        vmem((padded, 128), i32),
        vmem((padded, 128), f32),
        vmem((padded, width), bf16),
        vmem((chunks, 2, HALF, width), f32),
        vmem((ITERS, chunks, HALF, width), f32),
        vmem((ITERS, y_count, chunks, HALF // 2, width), i32),
        vmem((ITERS, y_count, chunks, 1, width), f32),
        vmem((ITERS, chunks, 2, HALF, 2 * width), bf16),
        vmem((padded, 2 * width), f32),
        vmem((2 * width, 2 * width), f32),
        vmem((n, padded // 128, 1, 128), f32),
        vmem((m, chunks, 1, CHUNK), f32),
        vmem((n * m, 1, 128), f32),
        vmem((ITERS, n, width // m, width), f32),
        vmem((ITERS, m, width // m, width), f32),
        vmem((m, width // m, width), f32),
        vmem((ITERS, n, piece // 2, width), i32),
        vmem((ITERS, n, 1, width), f32),
        vmem((ITERS, n, piece // 2, width), i32),
        vmem((ITERS, n, 1, width), f32),
        vmem((ITERS, n, piece // 2, width), i32),
        vmem((ITERS, n, 1, width), f32),
        vmem((width, width), f32),
        vmem((width, width), f32),
        vmem((width, width), f32),
        dma((chunks + 1,)),
        dma((2,)),
        dma((2,)),
        dma((2,)),
        dma((chunks + 1,)),
        dma((chunks + 1,)),
        dma((chunks + 1,)),
        dma((chunks + 1,)),
        dma((2,)),
        dma((2,)),
        dma((2,)),
        dma((2,)),
        dma((2,)),
        dma((2,)),
    ]
    basis, loadings = pl.pallas_call(
        functools.partial(body, n, m, gene_dev, math.sqrt(cell_count), gene_scale),
        out_shape=[jax.ShapeDtypeStruct((cell_dev, width), f32), jax.ShapeDtypeStruct((gene_dev, width), f32)],
        in_specs=[pl.BlockSpec(memory_space=pltpu.HBM)] * 2,
        out_specs=[pl.BlockSpec(memory_space=pltpu.VMEM)] * 2,
        scratch_shapes=scratch,
        compiler_params=pltpu.CompilerParams(
            collective_id=0, has_side_effects=True, vmem_limit_bytes=50 * 1024 * 1024
        ),
    )(table, sketch)
    return basis, loadings


def solution(mesh):
    return jax.shard_map(
        shards,
        mesh=mesh,
        in_specs=(P("cells", "genes"), P("genes", None)),
        out_specs=(P("cells", None), P("genes", None)),
        check_vma=False,
    )
```

```python
import functools
import math

import jax
import jax.numpy as jnp
from jax import lax
from jax.experimental import pallas as pl
from jax.experimental.pallas import tpu as pltpu
from jax.sharding import PartitionSpec as P

ITERS = 2
CHUNK = 256
HALF = CHUNK // 2
BLOCK = 64
DEPTH = 256
NEAR_LAG = 4
FIRST_PIECES = 5
BASIS_LAG = 4
CODE = 32767.0
MIDDLE = 32768.0
MESH = pl.DeviceIdType.MESH


def far_first(count):
    order = []
    for i in range((count + 1) // 2):
        order += [i] if 2 * i == count - 1 else [i, count - 1 - i]
    return order


def remote(src, dst, send_sem, recv_sem, peer):
    return pltpu.make_async_remote_copy(
        src_ref=src, dst_ref=dst, send_sem=send_sem, recv_sem=recv_sem, device_id=peer, device_id_type=MESH
    )


def encode(values):
    half = values.shape[0] // 2
    most = jnp.max(jnp.abs(values), axis=0, keepdims=True)
    inverse = jnp.where(most > 1e-30, CODE / most, 0.0)
    codes = (values * inverse + (MIDDLE + 0.5)).astype(jnp.int32)
    packed = codes[:half] | lax.shift_left(codes[half:], jnp.int32(16))
    return packed, most * (1.0 / CODE)


def decode(packed, unit):
    low = lax.bitwise_and(packed, jnp.int32(0xFFFF)).astype(jnp.float32)
    high = lax.shift_right_logical(packed, jnp.int32(16)).astype(jnp.float32)
    return jnp.concatenate([low - MIDDLE, high - MIDDLE], axis=0) * unit


def dot(left, right, left_dim, right_dim, precision=None):
    return lax.dot_general(
        left,
        right,
        (((left_dim,), (right_dim,)), ((), ())),
        precision=precision,
        preferred_element_type=jnp.float32,
    )


def split_terms(values):
    high = values.astype(jnp.bfloat16)
    return high, (values - high.astype(jnp.float32)).astype(jnp.bfloat16)


def whiten_start(gram, left, right):
    width = gram.shape[0]
    eye = lax.broadcasted_iota(jnp.int32, (width, width), 0) == lax.broadcasted_iota(jnp.int32, (width, width), 1)
    diagonal = jnp.where(eye, gram, 0.0)
    trace = jnp.sum(jnp.sum(diagonal, axis=1, keepdims=True), axis=0, keepdims=True)
    left[...] = gram + jnp.where(eye, 1e-05 * trace / width, 0.0)
    right[...] = jnp.where(eye, 1.0, 0.0)


def whiten_panels(start, stop, scale, out_ref, left, right):
    width = left.shape[0]
    place = lax.broadcasted_iota(jnp.int32, (8, width), 0)

    def spread(rows, step):
        return [jnp.broadcast_to(rows[:, 8 * step + i : 8 * step + i + 1], (8, width)) for i in range(8)]

    for step in range(start, stop):
        here = slice(8 * step, 8 * step + 8)
        rows_left, rows_right = left[here, :], right[here, :]
        columns = spread(rows_left, step)
        inverses, tops_left, tops_right, pivots = [], [], [], []
        done_right = jnp.zeros((8, width), jnp.float32)
        for i in range(8):
            inverse = lax.rsqrt(columns[i][i : i + 1, :])
            top_left, top_right = rows_left[i : i + 1, :] * inverse, rows_right[i : i + 1, :] * inverse
            done_right = jnp.where(place == i, top_right, done_right)
            factor = jnp.where(place > i, columns[i] * inverse, 0.0)
            rows_left = rows_left - factor * top_left
            rows_right = rows_right - factor * top_right
            pivot = {}
            for j in range(i + 1, 8):
                pivot[j] = columns[j][i : i + 1, :] * inverse
                columns[j] = columns[j] - factor * pivot[j]
            inverses.append(inverse)
            tops_left.append(top_left)
            tops_right.append(top_right)
            pivots.append(pivot)
        out_ref[here, :] = done_right * scale
        for block in range(step + 1, width // 8):
            there = slice(8 * block, 8 * block + 8)
            rows_left, rows_right = left[there, :], right[there, :]
            columns = spread(rows_left, step)
            for i in range(8):
                factor = columns[i] * inverses[i]
                rows_left = rows_left - factor * tops_left[i]
                rows_right = rows_right - factor * tops_right[i]
                for j in range(i + 1, 8):
                    columns[j] = columns[j] - factor * pivots[i][j]
            left[there, :] = rows_left
            right[there, :] = rows_right


def loop(count, body):
    lax.fori_loop(0, count, lambda i, carry: (body(i), carry)[1], 0)


def staged(count, lag, step):
    lag = min(lag, count)
    loop(lag, lambda i: step(i, True, False))
    lax.fori_loop(lag, count, lambda i, carry: (step(i, True, True), carry)[1], 0)
    lax.fori_loop(count, count + lag, lambda i, carry: (step(i, False, True), carry)[1], 0)


def body(
    n,
    m,
    gene_dev,
    limit,
    gene_scale,
    counts_ref,
    sketch_ref,
    basis_ref,
    load_ref,
    counts,
    resid,
    gene_acc,
    frac,
    omega,
    part,
    near,
    codes,
    units,
    terms,
    product,
    gram_acc,
    gene_all,
    cell_all,
    grand_all,
    gram_all,
    gram_rows,
    gram_part,
    gram_pair,
    load_part,
    load_part_unit,
    load_all,
    load_unit,
    load_sum,
    load_sum_unit,
    left,
    right,
    white,
    in_sem,
    gene_sem,
    cell_sem,
    grand_sem,
    near_sem,
    code_sem,
    unit_sem,
    term_sem,
    pair_sem,
    gram_sem,
    rows_sem,
    piece_sem,
    piece_unit_sem,
    all_sem,
    all_unit_sem,
):
    f32, bf16 = jnp.float32, jnp.bfloat16
    chunks, rows8, _ = counts.shape
    padded = resid.shape[1]
    width = left.shape[0]
    gene_rows = padded // 128
    cells_me, genes_me = lax.axis_index("cells"), lax.axis_index("genes")
    y_count = m // 2
    core, row = lax.rem(genes_me, 2), lax.div(genes_me, 2)
    partner = {"genes": row * 2 + 1 - core}
    y_peers = [{"genes": lax.rem(row + step, y_count) * 2 + core} for step in range(1, y_count)]
    beside = {"cells": lax.rem(cells_me + 1, n)}
    parity, level = lax.rem(cells_me, 2), lax.div(cells_me, 2)
    pair = {"cells": 2 * level + 1 - parity}

    def fetch(i):
        start = pl.multiple_of(i * CHUNK, CHUNK)
        return pltpu.make_async_copy(counts_ref.at[:, pl.ds(start, CHUNK)], counts.at[i], in_sem.at[i])

    loop(chunks, lambda i: fetch(i).start())
    sketch_copy = pltpu.make_async_copy(sketch_ref, omega.at[pl.ds(0, rows8)], in_sem.at[chunks])
    sketch_copy.start()
    barrier = pltpu.get_barrier_semaphore()

    def other(s):
        return {"cells": lax.rem(cells_me + lax.div(s, m), n), "genes": lax.rem(genes_me + lax.rem(s, m), m)}

    def greet(s):
        pl.semaphore_signal(barrier, inc=1, device_id=other(s + 1), device_id_type=MESH)

    loop(n * m - 1, greet)
    gene_acc[...] = jnp.zeros(gene_acc.shape, jnp.int32)
    if padded > rows8:
        omega[rows8:, :] = jnp.zeros((padded - rows8, width), bf16)
    step_rows = max(k for k in range(8, 65, 8) if rows8 % k == 0)

    def total_chunk(i):
        fetch(i).wait()

        def add(k, total):
            start = pl.ds(pl.multiple_of(k * step_rows, 8), step_rows)
            block = counts[i, start, :]
            gene_acc[start, :] += block[:, :HALF] + block[:, HALF:]
            for r in range(0, step_rows, 8):
                total = total + block[r : r + 8, :]
            return total

        total = lax.fori_loop(0, rows8 // step_rows, add, jnp.zeros((8, CHUNK), jnp.int32))
        cell_all[genes_me, i] = jnp.sum(total, axis=0, keepdims=True).astype(f32)

    with jax.named_scope("stream"):
        loop(chunks, total_chunk)
    for b in range(gene_rows):
        across = gene_acc[128 * b : 128 * (b + 1), :].astype(f32).T
        gene_row = jnp.sum(across, axis=0, keepdims=True)
        gene_all[cells_me, b] = gene_row
        grand = gene_row if b == 0 else grand + gene_row
    grand_all[cells_me * m + genes_me] = jnp.broadcast_to(jnp.sum(grand, axis=1, keepdims=True), (1, 128))
    with jax.named_scope("barrier"):
        pl.semaphore_wait(barrier, n * m - 1)

    def share(buffer, axis, me, sem):
        here = buffer.at[me]
        count = lax.axis_size(axis)
        for p in far_first(count):

            @pl.when(p != me)
            def _():
                remote(here, here, sem.at[0], sem.at[1], {axis: p}).start()

        everything = buffer.at[pl.ds(0, count - 1)]
        return remote(everything, everything, sem.at[0], sem.at[1], {axis: lax.rem(me + 1, count)})

    gene_copies = share(gene_all, "cells", cells_me, gene_sem)
    cell_copies = share(cell_all, "genes", genes_me, cell_sem)
    me = cells_me * m + genes_me

    def grand_start(s):
        here = grand_all.at[me]
        remote(here, here, grand_sem.at[0], grand_sem.at[1], other(s + 1)).start()

    loop(n * m - 1, grand_start)
    everything = grand_all.at[pl.ds(0, n * m - 1)]
    grand_copies = remote(everything, everything, grand_sem.at[0], grand_sem.at[1], other(1))
    with jax.named_scope("wait_gene"):
        gene_copies.wait_recv()
    gene_total = gene_all[0]
    for s in range(1, n):
        gene_total = gene_total + gene_all[s]
    with jax.named_scope("wait_grand"):
        grand_copies.wait_recv()
    grand = jnp.sum(grand_all[...], axis=0)
    for b in range(gene_rows):
        share_row = jnp.where(gene_total[b] > 0.0, gene_total[b] / grand, 1.0)
        frac[128 * b : 128 * (b + 1), :] = jnp.broadcast_to(share_row, (128, 128)).T
    with jax.named_scope("wait_cell"):
        cell_copies.wait_recv()

    def residual(i):
        cell_total = cell_all[0, i]
        for s in range(1, m):
            cell_total = cell_total + cell_all[s, i]
        sums = None
        for start in range(0, padded, DEPTH):
            stop = min(start + DEPTH, padded)
            blocks = []
            for k in range(start, min(stop, rows8), BLOCK):
                real = min(k + BLOCK, stop, rows8) - k
                share_of = frac[k : k + real, :]
                expected = jnp.concatenate([share_of, share_of], axis=1) * cell_total
                scaled = (counts[i, k : k + real, :].astype(f32) - expected) * lax.rsqrt(
                    expected + 0.01 * expected * expected
                )
                blocks.append(jnp.clip(scaled, -limit, limit))
            if stop > rows8:
                blocks.append(jnp.zeros((stop - max(start, rows8), CHUNK), f32))
            values = jnp.concatenate(blocks, axis=0).astype(bf16)
            resid[i, start:stop, :] = values
            term = dot(values, omega[start:stop, :], 0, 0)
            sums = term if sums is None else sums + term
        return sums

    sketch_copy.wait()
    for sweep in range(ITERS):

        def near_copy(i):
            return remote(part.at[i, 1 - core], near.at[sweep, i], near_sem.at[chunks], near_sem.at[i], partner)

        def code_start(i):
            for peer in y_peers:
                for buffer, sem in ((codes, code_sem), (units, unit_sem)):
                    here = buffer.at[sweep, row, i]
                    remote(here, here, sem.at[chunks], sem.at[i], peer).start()

        def code_wait(i):
            for buffer, sem in ((codes, code_sem), (units, unit_sem)):
                here = buffer.at[sweep, pl.ds(0, y_count - 1), i]
                remote(here, here, sem.at[chunks], sem.at[i], y_peers[0]).wait_recv()

        def term_copy(i):
            here = terms.at[sweep, i, core]
            return remote(here, here, term_sem.at[chunks], term_sem.at[i], partner)

        def first(i, sketch, code):
            j = i - NEAR_LAG
            if code:
                near_copy(j).wait_recv()
                packed, unit = encode(part[j, core] + near[sweep, j])
                codes[sweep, row, j] = packed
                units[sweep, row, j] = unit
            if sketch:
                rows = residual(i) if sweep == 0 else dot(resid[i], omega[...], 0, 0)
                part[i, 0] = rows[:HALF]
                part[i, 1] = rows[HALF:]
                near_copy(i).start()
            if code:
                code_start(j)

        def second(i, decoding, multiply):
            j = i - BASIS_LAG
            if decoding:
                code_wait(i)
            if multiply:
                term_copy(j).wait_recv()
                both = terms[sweep, j].reshape(CHUNK, 2 * width)
                gram_acc[...] += dot(both, both, 0, 0)
                product[...] += dot(resid[j], both, 1, 0)
            if decoding:
                total = decode(codes[sweep, 0, i], units[sweep, 0, i])
                for s in range(1, y_count):
                    total = total + decode(codes[sweep, s, i], units[sweep, s, i])
                high, low = split_terms(total)
                terms[sweep, i, core] = jnp.concatenate([high, low], axis=1)
                term_copy(i).start()

        with jax.named_scope(f"first{sweep}"):
            staged(chunks, NEAR_LAG, first)
        product[...] = jnp.zeros(product.shape, f32)
        gram_acc[...] = jnp.zeros(gram_acc.shape, f32)
        with jax.named_scope(f"second{sweep}"):
            staged(chunks, BASIS_LAG, second)

        gram = gram_acc[:width, :width] + gram_acc[:width, width:] + (gram_acc[width:, :width] + gram_acc[width:, width:])
        gram_part[...] = gram.reshape(gram_part.shape)
        pair_copy = remote(
            gram_part.at[genes_me, 1 - parity], gram_pair.at[sweep], pair_sem.at[0], pair_sem.at[1], pair
        )
        pair_copy.start()
        piece = padded // n
        piece_copies = []
        def level_sum():
            pair_copy.wait()
            gram_all[sweep, level] = gram_part[genes_me, parity] + gram_pair[sweep]
            for p in far_first(n // 2):
                here = gram_all.at[sweep, level]

                @pl.when(p != level)
                def _():
                    remote(here, here, gram_sem.at[0], gram_sem.at[1], {"cells": 2 * p + parity}).start()

            everything = gram_all.at[sweep, pl.ds(0, n // 2 - 1)]
            gram_copies = remote(everything, everything, gram_sem.at[0], gram_sem.at[1], beside)
            return gram_copies

        for step, p in enumerate(far_first(n)):
            if step == min(FIRST_PIECES, n - 1):
                gram_copies = level_sum()
            rows = product[p * piece : (p + 1) * piece, :]
            packed, unit = encode(rows[:, :width] + rows[:, width:])
            load_part[sweep, p] = packed
            load_part_unit[sweep, p] = unit

            @pl.when(p != cells_me)
            def _():
                for src, dst, sem in ((load_part, load_all, piece_sem), (load_part_unit, load_unit, piece_unit_sem)):
                    remote(src.at[sweep, p], dst.at[sweep, cells_me], sem.at[0], sem.at[1], {"cells": p}).start()

        load_all[sweep, cells_me] = load_part[sweep, cells_me]
        load_unit[sweep, cells_me] = load_part_unit[sweep, cells_me]
        for src, dst, sem in ((load_part, load_all, piece_sem), (load_part_unit, load_unit, piece_unit_sem)):
            most = pl.ds(0, n - 1)
            piece_copies.append(remote(src.at[sweep, most], dst.at[sweep, most], sem.at[0], sem.at[1], beside))
        with jax.named_scope(f"wait_gram{sweep}"):
            gram_copies.wait_recv()
        total = gram_all[sweep, 0]
        for s in range(1, n // 2):
            total = total + gram_all[sweep, s]
        mine = 2 * genes_me + parity
        gram_rows[sweep, mine] = total
        here = gram_rows.at[sweep, mine]
        for step in range(1, 2 * m):
            peer = {"genes": lax.rem(genes_me + step // 2, m)}
            if step % 2:
                peer["cells"] = pair["cells"]
            remote(here, here, rows_sem.at[0], rows_sem.at[1], peer).start()
        everything = gram_rows.at[sweep, pl.ds(0, 2 * m - 1)]
        rows_copies = remote(everything, everything, rows_sem.at[0], rows_sem.at[1], beside)
        with jax.named_scope(f"wait_piece{sweep}"):
            for copy in piece_copies:
                copy.wait_recv()
        total = decode(load_all[sweep, 0], load_unit[sweep, 0])
        for s in range(1, n):
            total = total + decode(load_all[sweep, s], load_unit[sweep, s])
        packed, unit = encode(total)
        load_sum[sweep, cells_me] = packed
        load_sum_unit[sweep, cells_me] = unit
        all_copies = share(load_sum.at[sweep], "cells", cells_me, all_sem)
        all_unit_copies = share(load_sum_unit.at[sweep], "cells", cells_me, all_unit_sem)
        with jax.named_scope(f"wait_rows{sweep}"):
            rows_copies.wait_recv()
        scale = math.sqrt(chunks * CHUNK * n)
        with jax.named_scope(f"whiten{sweep}"):
            whiten_start(gram_rows[sweep].reshape(width, width), left, right)
            whiten_panels(0, width // 8, scale, white, left, right)
        last = sweep == ITERS - 1
        high, low = split_terms(white[...].T)
        wide = jnp.concatenate([high, low], axis=1)
        wide = jnp.concatenate([wide, wide], axis=0)
        if last:

            def write(i):
                rows = dot(terms[sweep, i].reshape(CHUNK, 2 * width), wide, 1, 0)
                start = pl.multiple_of(i * CHUNK, CHUNK)
                basis_ref[pl.ds(start, CHUNK), :] = rows[:, :width] + rows[:, width:]

            with jax.named_scope("write"):
                lax.fori_loop(0, chunks, lambda i, carry: (write(i), carry)[1], 0, unroll=True)
        with jax.named_scope(f"wait_all{sweep}"):
            all_copies.wait_recv()
            all_unit_copies.wait_recv()
        with jax.named_scope(f"loads{sweep}"):
            for p in range(n):
                high, low = split_terms(decode(load_sum[sweep, p], load_sum_unit[sweep, p]))
                loads = dot(jnp.concatenate([high, low], axis=1), wide, 1, 0)
                loads = (loads[:, :width] + loads[:, width:]) * gene_scale
                start, stop = piece * p, min(piece * (p + 1), gene_dev)
                if last and stop > start:
                    load_ref[start:stop, :] = loads[: stop - start]
                elif not last:
                    omega[start : piece * (p + 1), :] = loads.astype(bf16)
        for copies in [gram_copies, rows_copies, all_copies, all_unit_copies] + piece_copies:
            copies.wait_send()
        near_all, term_all = near.at[sweep], terms.at[sweep, pl.ds(0, chunks), core]
        remote(near_all, near_all, near_sem.at[chunks], near_sem.at[0], partner).wait_send()
        remote(term_all, term_all, term_sem.at[chunks], term_sem.at[0], partner).wait_send()
        for buffer, sem in ((codes, code_sem), (units, unit_sem)):
            here = buffer.at[sweep, pl.ds(0, y_count - 1)]
            remote(here, here, sem.at[chunks], sem.at[0], y_peers[0]).wait_send()
    for copies in (gene_copies, cell_copies, grand_copies):
        copies.wait_send()


def shards(counts, sketch):
    cell_dev, gene_dev = counts.shape
    n, m = lax.axis_size("cells"), lax.axis_size("genes")
    width = sketch.shape[1]
    rows8 = -(-gene_dev // 8) * 8
    unit = max(16 * n, 128)
    padded = -(-gene_dev // unit) * unit
    chunks = cell_dev // CHUNK
    strip = width // (2 * m)
    assert chunks * CHUNK == cell_dev and m % 2 == 0 and n % 2 == 0 and strip % 8 == 0
    table = counts.T
    if rows8 > gene_dev:
        table = jnp.pad(table, ((0, rows8 - gene_dev), (0, 0)))
        sketch = jnp.pad(sketch, ((0, rows8 - gene_dev), (0, 0)))
    cell_count = float(cell_dev * n)
    gene_scale = math.sqrt(float(gene_dev * m)) / cell_count
    f32, bf16, i32 = jnp.float32, jnp.bfloat16, jnp.int32
    y_count = m // 2
    piece = padded // n
    vmem = pltpu.VMEM
    dma = pltpu.SemaphoreType.DMA
    scratch = [
        vmem((chunks, rows8, CHUNK), i32),
        vmem((chunks, padded, CHUNK), bf16),
        vmem((padded, 128), i32),
        vmem((padded, 128), f32),
        vmem((padded, width), bf16),
        vmem((chunks, 2, HALF, width), f32),
        vmem((ITERS, chunks, HALF, width), f32),
        vmem((ITERS, y_count, chunks, HALF // 2, width), i32),
        vmem((ITERS, y_count, chunks, 1, width), f32),
        vmem((ITERS, chunks, 2, HALF, 2 * width), bf16),
        vmem((padded, 2 * width), f32),
        vmem((2 * width, 2 * width), f32),
        vmem((n, padded // 128, 1, 128), f32),
        vmem((m, chunks, 1, CHUNK), f32),
        vmem((n * m, 1, 128), f32),
        vmem((ITERS, n // 2, strip, width), f32),
        vmem((ITERS, 2 * m, strip, width), f32),
        vmem((m, 2, strip, width), f32),
        vmem((ITERS, strip, width), f32),
        vmem((ITERS, n, piece // 2, width), i32),
        vmem((ITERS, n, 1, width), f32),
        vmem((ITERS, n, piece // 2, width), i32),
        vmem((ITERS, n, 1, width), f32),
        vmem((ITERS, n, piece // 2, width), i32),
        vmem((ITERS, n, 1, width), f32),
        vmem((width, width), f32),
        vmem((width, width), f32),
        vmem((width, width), f32),
        dma((chunks + 1,)),
        dma((2,)),
        dma((2,)),
        dma((2,)),
        dma((chunks + 1,)),
        dma((chunks + 1,)),
        dma((chunks + 1,)),
        dma((chunks + 1,)),
        dma((2,)),
        dma((2,)),
        dma((2,)),
        dma((2,)),
        dma((2,)),
        dma((2,)),
        dma((2,)),
    ]
    basis, loadings = pl.pallas_call(
        functools.partial(body, n, m, gene_dev, math.sqrt(cell_count), gene_scale),
        out_shape=[jax.ShapeDtypeStruct((cell_dev, width), f32), jax.ShapeDtypeStruct((gene_dev, width), f32)],
        in_specs=[pl.BlockSpec(memory_space=pltpu.HBM)] * 2,
        out_specs=[pl.BlockSpec(memory_space=pltpu.VMEM)] * 2,
        scratch_shapes=scratch,
        compiler_params=pltpu.CompilerParams(
            collective_id=0, has_side_effects=True, vmem_limit_bytes=50 * 1024 * 1024
        ),
    )(table, sketch)
    return basis, loadings


def solution(mesh):
    return jax.shard_map(
        shards,
        mesh=mesh,
        in_specs=(P("cells", "genes"), P("genes", None)),
        out_specs=(P("cells", None), P("genes", None)),
        check_vma=False,
    )
```

```python
import functools
import math

import jax
import jax.numpy as jnp
from jax import lax
from jax.experimental import pallas as pl
from jax.experimental.pallas import tpu as pltpu
from jax.sharding import PartitionSpec as P

ITERS = 2
CHUNK = 256
HALF = CHUNK // 2
BLOCK = 64
DEPTH = 128
NEAR_LAG = 4
GROUP = 5
FIRST_PIECES = 5
BASIS_LAG = 4
CODE = 32767.0
MIDDLE = 32768.0
MESH = pl.DeviceIdType.MESH


def far_first(count):
    order = []
    for i in range((count + 1) // 2):
        order += [i] if 2 * i == count - 1 else [i, count - 1 - i]
    return order


def remote(src, dst, send_sem, recv_sem, peer):
    return pltpu.make_async_remote_copy(
        src_ref=src, dst_ref=dst, send_sem=send_sem, recv_sem=recv_sem, device_id=peer, device_id_type=MESH
    )


def encode(values):
    half = values.shape[0] // 2
    most = jnp.max(jnp.abs(values), axis=0, keepdims=True)
    inverse = jnp.where(most > 1e-30, CODE / most, 0.0)
    codes = (values * inverse + (MIDDLE + 0.5)).astype(jnp.int32)
    packed = codes[:half] | lax.shift_left(codes[half:], jnp.int32(16))
    return packed, most * (1.0 / CODE)


def decode(packed, unit):
    low = lax.bitwise_and(packed, jnp.int32(0xFFFF)).astype(jnp.float32)
    high = lax.shift_right_logical(packed, jnp.int32(16)).astype(jnp.float32)
    return jnp.concatenate([low - MIDDLE, high - MIDDLE], axis=0) * unit


def dot(left, right, left_dim, right_dim, precision=None):
    return lax.dot_general(
        left,
        right,
        (((left_dim,), (right_dim,)), ((), ())),
        precision=precision,
        preferred_element_type=jnp.float32,
    )


def split_terms(values):
    high = values.astype(jnp.bfloat16)
    return high, (values - high.astype(jnp.float32)).astype(jnp.bfloat16)


def whiten_start(gram, left, right):
    width = gram.shape[0]
    eye = lax.broadcasted_iota(jnp.int32, (width, width), 0) == lax.broadcasted_iota(jnp.int32, (width, width), 1)
    diagonal = jnp.where(eye, gram, 0.0)
    trace = jnp.sum(jnp.sum(diagonal, axis=1, keepdims=True), axis=0, keepdims=True)
    left[...] = gram + jnp.where(eye, 1e-05 * trace / width, 0.0)
    right[...] = jnp.where(eye, 1.0, 0.0)


def whiten_panels(start, stop, scale, out_ref, left, right):
    width = left.shape[0]
    place = lax.broadcasted_iota(jnp.int32, (8, width), 0)

    def spread(rows, step):
        return [jnp.broadcast_to(rows[:, 8 * step + i : 8 * step + i + 1], (8, width)) for i in range(8)]

    ahead = []
    for step in range(start, stop):
        here = slice(8 * step, 8 * step + 8)
        rows_left, rows_right = left[here, :], right[here, :]
        columns = ahead if ahead else spread(rows_left, step)
        inverses, tops_left, tops_right, pivots = [], [], [], []
        ahead = []
        done_right = jnp.zeros((8, width), jnp.float32)
        for i in range(8):
            inverse = lax.rsqrt(columns[i][i : i + 1, :])
            top_left, top_right = rows_left[i : i + 1, :] * inverse, rows_right[i : i + 1, :] * inverse
            done_right = jnp.where(place == i, top_right, done_right)
            factor = jnp.where(place > i, columns[i] * inverse, 0.0)
            rows_left = rows_left - factor * top_left
            rows_right = rows_right - factor * top_right
            pivot = {}
            for j in range(i + 1, 8):
                pivot[j] = columns[j][i : i + 1, :] * inverse
                columns[j] = columns[j] - factor * pivot[j]
            inverses.append(inverse)
            tops_left.append(top_left)
            tops_right.append(top_right)
            pivots.append(pivot)
        out_ref[here, :] = done_right * scale
        for block in range(step + 1, width // 8):
            there = slice(8 * block, 8 * block + 8)
            rows_left, rows_right = left[there, :], right[there, :]
            columns = spread(rows_left, step)
            if block == step + 1:
                ahead = spread(rows_left, block)
            for i in range(8):
                factor = columns[i] * inverses[i]
                if block == step + 1:
                    ahead = [ahead[j] - factor * factor[j : j + 1, :] for j in range(8)]
                rows_left = rows_left - factor * tops_left[i]
                rows_right = rows_right - factor * tops_right[i]
                for j in range(i + 1, 8):
                    columns[j] = columns[j] - factor * pivots[i][j]
            left[there, :] = rows_left
            right[there, :] = rows_right


def loop(count, body):
    lax.fori_loop(0, count, lambda i, carry: (body(i), carry)[1], 0)


def staged(count, lag, step):
    lag = min(lag, count)
    loop(lag, lambda i: step(i, True, False))
    lax.fori_loop(lag, count, lambda i, carry: (step(i, True, True), carry)[1], 0)
    lax.fori_loop(count, count + lag, lambda i, carry: (step(i, False, True), carry)[1], 0)


def two_term_loads(packed, unit, wide):
    high, low = split_terms(decode(packed, unit))
    loads = dot(jnp.concatenate([high, low], axis=1), wide, 1, 0)
    half = loads.shape[1] // 2
    return loads[:, :half] + loads[:, half:]


def write_body(
    gene_dev, gene_scale, terms, wide_ref, sums, units, basis_out, load_out, basis, loadings, basis_sem, load_sem
):
    chunks = terms.shape[0]
    width = basis.shape[1]
    wide = wide_ref[...]
    parts, members, part_rows, _ = sums.shape
    copies = []
    for p in range(members):
        for q in range(parts):
            start = 2 * part_rows * (p * parts + q)
            stop = min(start + 2 * part_rows, gene_dev)
            if stop > start:
                loads = two_term_loads(sums[q, p], units[q, p], wide) * gene_scale
                loadings[start:stop, :] = loads[: stop - start]
    copies.append(pltpu.make_async_copy(loadings, load_out, load_sem))
    copies[0].start()
    for k, start in enumerate(range(0, chunks, GROUP)):
        stop = min(start + GROUP, chunks)
        for i in range(start, stop):
            rows = dot(terms[i].reshape(CHUNK, 2 * width), wide, 1, 0)
            basis[i * CHUNK : (i + 1) * CHUNK, :] = rows[:, :width] + rows[:, width:]
        rows = pl.ds(start * CHUNK, (stop - start) * CHUNK)
        copies.append(pltpu.make_async_copy(basis.at[rows], basis_out.at[rows], basis_sem.at[k]))
        copies[-1].start()
    for copy in copies:
        copy.wait()


def body(
    n,
    m,
    gene_dev,
    limit,
    gene_scale,
    counts_ref,
    sketch_ref,
    last_terms,
    wide_ref,
    last_sum,
    last_unit,
    counts,
    resid,
    gene_acc,
    frac,
    omega,
    part,
    near,
    codes,
    units,
    first_terms,
    product,
    gram_acc,
    gene_all,
    cell_all,
    grand_all,
    gram_all,
    gram_rows,
    gram_part,
    gram_pair,
    load_part,
    load_part_unit,
    load_all,
    load_unit,
    swap,
    swap_unit,
    first_sum,
    first_unit,
    left,
    right,
    white,
    in_sem,
    gene_sem,
    cell_sem,
    grand_sem,
    near_sem,
    code_sem,
    unit_sem,
    term_sem,
    pair_sem,
    gram_sem,
    rows_sem,
    piece_sem,
    piece_unit_sem,
    swap_sem,
    swap_unit_sem,
    all_sem,
    all_unit_sem,
):
    f32, bf16 = jnp.float32, jnp.bfloat16
    chunks, rows8, _ = counts.shape
    parts = load_all.shape[1]
    padded = resid.shape[1]
    width = left.shape[0]
    gene_rows = padded // 128
    cells_me, genes_me = lax.axis_index("cells"), lax.axis_index("genes")
    y_count = m // 2
    core, row = lax.rem(genes_me, 2), lax.div(genes_me, 2)
    partner = {"genes": row * 2 + 1 - core}
    y_peers = [{"genes": lax.rem(row + step, y_count) * 2 + core} for step in range(1, y_count)]
    beside = {"cells": lax.rem(cells_me + 1, n)}
    parity, level = lax.rem(cells_me, 2), lax.div(cells_me, 2)
    pair = {"cells": 2 * level + 1 - parity}

    def fetch(i):
        start = pl.multiple_of(i * CHUNK, CHUNK)
        return pltpu.make_async_copy(counts_ref.at[:, pl.ds(start, CHUNK)], counts.at[i], in_sem.at[i])

    loop(chunks, lambda i: fetch(i).start())
    sketch_copy = pltpu.make_async_copy(sketch_ref, omega.at[pl.ds(0, rows8)], in_sem.at[chunks])
    sketch_copy.start()
    barrier = pltpu.get_barrier_semaphore()

    def other(s):
        return {"cells": lax.rem(cells_me + lax.div(s, m), n), "genes": lax.rem(genes_me + lax.rem(s, m), m)}

    def greet(s):
        pl.semaphore_signal(barrier, inc=1, device_id=other(s + 1), device_id_type=MESH)

    loop(n * m - 1, greet)
    gene_acc[...] = jnp.zeros(gene_acc.shape, jnp.int32)
    if padded > rows8:
        omega[rows8:, :] = jnp.zeros((padded - rows8, width), bf16)
    step_rows = max(k for k in range(8, 65, 8) if rows8 % k == 0)

    def total_chunk(i):
        fetch(i).wait()

        def add(k, total):
            start = pl.ds(pl.multiple_of(k * step_rows, 8), step_rows)
            block = counts[i, start, :]
            gene_acc[start, :] += block[:, :HALF] + block[:, HALF:]
            for r in range(0, step_rows, 8):
                total = total + block[r : r + 8, :]
            return total

        total = lax.fori_loop(0, rows8 // step_rows, add, jnp.zeros((8, CHUNK), jnp.int32))
        cell_all[genes_me, i] = jnp.sum(total, axis=0, keepdims=True).astype(f32)

    with jax.named_scope("stream"):
        loop(chunks, total_chunk)
    for b in range(gene_rows):
        across = gene_acc[128 * b : 128 * (b + 1), :].astype(f32).T
        gene_row = jnp.sum(across, axis=0, keepdims=True)
        gene_all[cells_me, b] = gene_row
        grand = gene_row if b == 0 else grand + gene_row
    grand_all[cells_me * m + genes_me] = jnp.broadcast_to(jnp.sum(grand, axis=1, keepdims=True), (1, 128))
    with jax.named_scope("barrier"):
        pl.semaphore_wait(barrier, n * m - 1)

    def share(buffer, axis, me, sem):
        here = buffer.at[me]
        count = lax.axis_size(axis)
        for p in far_first(count):

            @pl.when(p != me)
            def _():
                remote(here, here, sem.at[0], sem.at[1], {axis: p}).start()

        everything = buffer.at[pl.ds(0, count - 1)]
        return remote(everything, everything, sem.at[0], sem.at[1], {axis: lax.rem(me + 1, count)})

    gene_copies = share(gene_all, "cells", cells_me, gene_sem)
    cell_copies = share(cell_all, "genes", genes_me, cell_sem)
    me = cells_me * m + genes_me

    def grand_start(s):
        here = grand_all.at[me]
        remote(here, here, grand_sem.at[0], grand_sem.at[1], other(s + 1)).start()

    loop(n * m - 1, grand_start)
    everything = grand_all.at[pl.ds(0, n * m - 1)]
    grand_copies = remote(everything, everything, grand_sem.at[0], grand_sem.at[1], other(1))
    with jax.named_scope("wait_gene"):
        gene_copies.wait_recv()
    gene_total = gene_all[0]
    for s in range(1, n):
        gene_total = gene_total + gene_all[s]
    with jax.named_scope("wait_grand"):
        grand_copies.wait_recv()
    grand = jnp.sum(grand_all[...], axis=0)
    for b in range(gene_rows):
        share_row = jnp.where(gene_total[b] > 0.0, gene_total[b] / grand, 1.0)
        frac[128 * b : 128 * (b + 1), :] = jnp.broadcast_to(share_row, (128, 128)).T
    with jax.named_scope("wait_cell"):
        cell_copies.wait_recv()

    low_limit, high_limit = jnp.asarray(-limit, bf16), jnp.asarray(limit, bf16)

    def residual(i):
        cell_total = cell_all[0, i]
        for s in range(1, m):
            cell_total = cell_total + cell_all[s, i]
        sums = None
        for start in range(0, padded, DEPTH):
            stop = min(start + DEPTH, padded)
            blocks = []
            for k in range(start, min(stop, rows8), BLOCK):
                real = min(k + BLOCK, stop, rows8) - k
                share_of = frac[k : k + real, :]
                expected = jnp.concatenate([share_of, share_of], axis=1) * cell_total
                scaled = (counts[i, k : k + real, :].astype(f32) - expected) * lax.rsqrt(
                    expected + 0.01 * expected * expected
                )
                blocks.append(scaled)
            if stop > rows8:
                blocks.append(jnp.zeros((stop - max(start, rows8), CHUNK), f32))
            values = jnp.clip(jnp.concatenate(blocks, axis=0).astype(bf16), low_limit, high_limit)
            resid[i, start:stop, :] = values
            term = dot(values, omega[start:stop, :], 0, 0)
            sums = term if sums is None else sums + term
        return sums

    sketch_copy.wait()
    for sweep in range(ITERS):
        last = sweep == ITERS - 1
        terms = last_terms if last else first_terms
        load_sum, load_sum_unit = (last_sum, last_unit) if last else (first_sum, first_unit)

        def near_copy(i):
            return remote(part.at[i, 1 - core], near.at[sweep, i], near_sem.at[chunks], near_sem.at[i], partner)

        def code_start(i):
            for peer in y_peers:
                for buffer, sem in ((codes, code_sem), (units, unit_sem)):
                    here = buffer.at[sweep, row, i]
                    remote(here, here, sem.at[chunks], sem.at[i], peer).start()

        def code_wait(i):
            for buffer, sem in ((codes, code_sem), (units, unit_sem)):
                here = buffer.at[sweep, pl.ds(0, y_count - 1), i]
                remote(here, here, sem.at[chunks], sem.at[i], y_peers[0]).wait_recv()

        def term_copy(i):
            here = terms.at[i, core]
            return remote(here, here, term_sem.at[chunks], term_sem.at[i], partner)

        def first(i, sketch, code):
            j = i - NEAR_LAG
            if code:
                near_copy(j).wait_recv()
                packed, unit = encode(part[j, core] + near[sweep, j])
                codes[sweep, row, j] = packed
                units[sweep, row, j] = unit
            if sketch:
                rows = residual(i) if sweep == 0 else dot(resid[i], omega[...], 0, 0)
                part[i, 0] = rows[:HALF]
                part[i, 1] = rows[HALF:]
                near_copy(i).start()
            if code:
                code_start(j)

        def second(i, decoding, multiply):
            j = i - BASIS_LAG
            if decoding:
                code_wait(i)
            if multiply:
                term_copy(j).wait_recv()
                both = terms[j].reshape(CHUNK, 2 * width)
                gram_acc[...] += dot(both, both, 0, 0)
                product[...] += dot(resid[j], both, 1, 0)
            if decoding:
                total = decode(codes[sweep, 0, i], units[sweep, 0, i])
                for s in range(1, y_count):
                    total = total + decode(codes[sweep, s, i], units[sweep, s, i])
                high, low = split_terms(total)
                terms[i, core] = jnp.concatenate([high, low], axis=1)
                term_copy(i).start()

        with jax.named_scope(f"first{sweep}"):
            staged(chunks, NEAR_LAG, first)
        product[...] = jnp.zeros(product.shape, f32)
        gram_acc[...] = jnp.zeros(gram_acc.shape, f32)
        with jax.named_scope(f"second{sweep}"):
            staged(chunks, BASIS_LAG, second)

        gram = gram_acc[:width, :width] + gram_acc[:width, width:] + (gram_acc[width:, :width] + gram_acc[width:, width:])
        gram_part[...] = gram.reshape(gram_part.shape)
        pair_copy = remote(
            gram_part.at[genes_me, 1 - parity], gram_pair.at[sweep], pair_sem.at[sweep, 0], pair_sem.at[sweep, 1], pair
        )
        pair_copy.start()
        members = n // 2
        piece = padded // members
        part_rows = piece // 2 // parts
        side, member = lax.div(cells_me, members), lax.rem(cells_me, members)
        across = {"cells": (1 - side) * members + member}
        stage_sems = ((load_all, piece_sem), (load_unit, piece_unit_sem))

        def scatter(q):
            for p in range(members):
                start = p * piece + q * 2 * part_rows
                rows = product[start : start + 2 * part_rows, :]
                packed, unit = encode(rows[:, :width] + rows[:, width:])
                load_part[sweep, q, p] = packed
                load_part_unit[sweep, q, p] = unit

                @pl.when(p != member)
                def _():
                    for src, (dst, sem) in zip((load_part, load_part_unit), stage_sems):
                        sems = sem.at[q, 0], sem.at[q, 1]
                        remote(
                            src.at[sweep, q, p], dst.at[sweep, q, member], *sems, {"cells": side * members + p}
                        ).start()

            load_all[sweep, q, member] = load_part[sweep, q, member]
            load_unit[sweep, q, member] = load_part_unit[sweep, q, member]

        def most_of(buffer, sem):
            most = buffer.at[pl.ds(0, members - 1)]
            return remote(most, most, sem.at[0], sem.at[1], across)

        piece_copies = [
            most_of(dst.at[sweep, q], sem.at[q]) for q in range(parts) for dst, sem in stage_sems
        ]

        def swap_copies(q):
            return [
                remote(buffer.at[sweep, q, side], buffer.at[sweep, q, side], sem.at[sweep, q, 0], sem.at[sweep, q, 1], across)
                for buffer, sem in ((swap, swap_sem), (swap_unit, swap_unit_sem))
            ]

        def cross(q):
            with jax.named_scope(f"wait_piece{q}{sweep}"):
                piece_copies[2 * q].wait_recv()
                piece_copies[2 * q + 1].wait_recv()
            total = decode(load_all[sweep, q, 0], load_unit[sweep, q, 0])
            for s in range(1, members):
                total = total + decode(load_all[sweep, q, s], load_unit[sweep, q, s])
            packed, unit = encode(total)
            swap[sweep, q, side] = packed
            swap_unit[sweep, q, side] = unit
            for copy in swap_copies(q):
                copy.start()

        all_copies = []

        def gather(q):
            with jax.named_scope(f"wait_swap{q}{sweep}"):
                for copy in swap_copies(q):
                    copy.wait_recv()
            total = decode(swap[sweep, q, 0], swap_unit[sweep, q, 0])
            total = total + decode(swap[sweep, q, 1], swap_unit[sweep, q, 1])
            packed, unit = encode(total)
            load_sum[q, member] = packed
            load_sum_unit[q, member] = unit
            for buffer, sem in ((load_sum, all_sem), (load_sum_unit, all_unit_sem)):
                here = buffer.at[q, member]
                for p in range(members):

                    @pl.when(p != member)
                    def _():
                        remote(here, here, sem.at[q, 0], sem.at[q, 1], {"cells": side * members + p}).start()

                all_copies.append(most_of(buffer.at[q], sem.at[q]))

        def level_sum():
            pair_copy.wait()
            gram_all[sweep, level] = gram_part[genes_me, parity] + gram_pair[sweep]
            for p in far_first(n // 2):
                here = gram_all.at[sweep, level]

                @pl.when(p != level)
                def _():
                    remote(here, here, gram_sem.at[sweep, 0], gram_sem.at[sweep, 1], {"cells": 2 * p + parity}).start()

            everything = gram_all.at[sweep, pl.ds(0, n // 2 - 1)]
            gram_copies = remote(everything, everything, gram_sem.at[sweep, 0], gram_sem.at[sweep, 1], beside)
            return gram_copies

        for q in range(parts):
            scatter(q)
        gram_copies = level_sum()
        for q in range(parts):
            cross(q)
        with jax.named_scope(f"wait_gram{sweep}"):
            gram_copies.wait_recv()
        total = gram_all[sweep, 0]
        for s in range(1, n // 2):
            total = total + gram_all[sweep, s]
        mine = 2 * genes_me + parity
        gram_rows[sweep, mine] = total
        here = gram_rows.at[sweep, mine]
        for step in range(1, 2 * m):
            peer = {"genes": lax.rem(genes_me + step // 2, m)}
            if step % 2:
                peer["cells"] = pair["cells"]
            remote(here, here, rows_sem.at[sweep, 0], rows_sem.at[sweep, 1], peer).start()
        everything = gram_rows.at[sweep, pl.ds(0, 2 * m - 1)]
        rows_copies = remote(everything, everything, rows_sem.at[sweep, 0], rows_sem.at[sweep, 1], beside)
        for q in range(parts):
            gather(q)
        with jax.named_scope(f"wait_rows{sweep}"):
            rows_copies.wait_recv()
        scale = math.sqrt(chunks * CHUNK * n)
        with jax.named_scope(f"whiten{sweep}"):
            whiten_start(gram_rows[sweep].reshape(width, width), left, right)
            whiten_panels(0, width // 8, scale, white, left, right)
        high, low = split_terms(white[...].T)
        wide = jnp.concatenate([high, low], axis=1)
        wide = jnp.concatenate([wide, wide], axis=0)
        if last:
            wide_ref[...] = wide
        with jax.named_scope(f"wait_all{sweep}"):
            for copies in all_copies:
                copies.wait_recv()
        if not last:
            for p in range(members):
                for q in range(parts):
                    loads = two_term_loads(load_sum[q, p], load_sum_unit[q, p], wide)
                    start = piece * p + 2 * part_rows * q
                    omega[start : start + 2 * part_rows, :] = (loads * gene_scale).astype(bf16)
        for copies in [gram_copies, rows_copies] + all_copies + piece_copies + swap_copies(0) + swap_copies(parts - 1)[: 2 * (parts - 1)]:
            copies.wait_send()
        near_all, term_all = near.at[sweep], terms.at[pl.ds(0, chunks), core]
        remote(near_all, near_all, near_sem.at[chunks], near_sem.at[0], partner).wait_send()
        remote(term_all, term_all, term_sem.at[chunks], term_sem.at[0], partner).wait_send()
        for buffer, sem in ((codes, code_sem), (units, unit_sem)):
            here = buffer.at[sweep, pl.ds(0, y_count - 1)]
            remote(here, here, sem.at[chunks], sem.at[0], y_peers[0]).wait_send()
    for copies in (gene_copies, cell_copies, grand_copies):
        copies.wait_send()


def shards(counts, sketch):
    cell_dev, gene_dev = counts.shape
    n, m = lax.axis_size("cells"), lax.axis_size("genes")
    width = sketch.shape[1]
    rows8 = -(-gene_dev // 8) * 8
    unit = max(16 * n, 128)
    padded = -(-gene_dev // unit) * unit
    chunks = cell_dev // CHUNK
    strip = width // (2 * m)
    assert chunks * CHUNK == cell_dev and m % 2 == 0 and n % 2 == 0 and strip % 8 == 0
    table = counts.T
    if rows8 > gene_dev:
        table = jnp.pad(table, ((0, rows8 - gene_dev), (0, 0)))
        sketch = jnp.pad(sketch, ((0, rows8 - gene_dev), (0, 0)))
    cell_count = float(cell_dev * n)
    gene_scale = math.sqrt(float(gene_dev * m)) / cell_count
    f32, bf16, i32 = jnp.float32, jnp.bfloat16, jnp.int32
    y_count = m // 2
    members = n // 2
    piece = padded // members
    parts = 2 if piece % 32 == 0 else 1
    part_rows = piece // 2 // parts
    vmem = pltpu.VMEM
    dma = pltpu.SemaphoreType.DMA
    scratch = [
        vmem((chunks, rows8, CHUNK), i32),
        vmem((chunks, padded, CHUNK), bf16),
        vmem((padded, 128), i32),
        vmem((padded, 128), f32),
        vmem((padded, width), bf16),
        vmem((chunks, 2, HALF, width), f32),
        vmem((ITERS, chunks, HALF, width), f32),
        vmem((ITERS, y_count, chunks, HALF // 2, width), i32),
        vmem((ITERS, y_count, chunks, 1, width), f32),
        vmem((chunks, 2, HALF, 2 * width), bf16),
        vmem((padded, 2 * width), f32),
        vmem((2 * width, 2 * width), f32),
        vmem((n, padded // 128, 1, 128), f32),
        vmem((m, chunks, 1, CHUNK), f32),
        vmem((n * m, 1, 128), f32),
        vmem((ITERS, n // 2, strip, width), f32),
        vmem((ITERS, 2 * m, strip, width), f32),
        vmem((m, 2, strip, width), f32),
        vmem((ITERS, strip, width), f32),
        vmem((ITERS, parts, members, part_rows, width), i32),
        vmem((ITERS, parts, members, 1, width), f32),
        vmem((ITERS, parts, members, part_rows, width), i32),
        vmem((ITERS, parts, members, 1, width), f32),
        vmem((ITERS, parts, 2, part_rows, width), i32),
        vmem((ITERS, parts, 2, 1, width), f32),
        vmem((parts, members, part_rows, width), i32),
        vmem((parts, members, 1, width), f32),
        vmem((width, width), f32),
        vmem((width, width), f32),
        vmem((width, width), f32),
        dma((chunks + 1,)),
        dma((2,)),
        dma((2,)),
        dma((2,)),
        dma((chunks + 1,)),
        dma((chunks + 1,)),
        dma((chunks + 1,)),
        dma((chunks + 1,)),
        dma((ITERS, 2)),
        dma((ITERS, 2)),
        dma((ITERS, 2)),
        dma((parts, 2)),
        dma((parts, 2)),
        dma((ITERS, parts, 2)),
        dma((ITERS, parts, 2)),
        dma((parts, 2)),
        dma((parts, 2)),
    ]
    handed = [
        jax.ShapeDtypeStruct((chunks, 2, HALF, 2 * width), bf16),
        jax.ShapeDtypeStruct((2 * width, 2 * width), bf16),
        jax.ShapeDtypeStruct((parts, members, part_rows, width), i32),
        jax.ShapeDtypeStruct((parts, members, 1, width), f32),
    ]
    handed = pl.pallas_call(
        functools.partial(body, n, m, gene_dev, math.sqrt(cell_count), gene_scale),
        out_shape=handed,
        in_specs=[pl.BlockSpec(memory_space=pltpu.HBM)] * 2,
        out_specs=[pl.BlockSpec(memory_space=pltpu.VMEM)] * 4,
        scratch_shapes=scratch,
        compiler_params=pltpu.CompilerParams(
            collective_id=0, has_side_effects=True, vmem_limit_bytes=48 * 1024 * 1024
        ),
    )(table, sketch)
    return pl.pallas_call(
        functools.partial(write_body, gene_dev, gene_scale),
        out_shape=[jax.ShapeDtypeStruct((cell_dev, width), f32), jax.ShapeDtypeStruct((gene_dev, width), f32)],
        in_specs=[pl.BlockSpec(memory_space=pltpu.VMEM)] * 4,
        out_specs=[pl.BlockSpec(memory_space=pltpu.HBM)] * 2,
        scratch_shapes=[
            vmem((cell_dev, width), f32),
            vmem((gene_dev, width), f32),
            dma((-(-chunks // GROUP),)),
            dma(()),
        ],
        compiler_params=pltpu.CompilerParams(vmem_limit_bytes=16 * 1024 * 1024),
    )(*handed)


def solution(mesh):
    return jax.shard_map(
        shards,
        mesh=mesh,
        in_specs=(P("cells", "genes"), P("genes", None)),
        out_specs=(P("cells", None), P("genes", None)),
        check_vma=False,
    )
```

```python
import functools
import math

import jax
import jax.numpy as jnp
from jax import lax
from jax.experimental import pallas as pl
from jax.experimental.pallas import tpu as pltpu
from jax.sharding import PartitionSpec as P

ITERS = 2
CHUNK = 256
HALF = CHUNK // 2
BLOCK = 64
DEPTH = 128
NEAR_LAG = 4
GROUP = 4
FIRST_PIECES = 5
BASIS_LAG = 4
CODE = 32767.0
MIDDLE = 32768.0
MESH = pl.DeviceIdType.MESH


def far_first(count):
    order = []
    for i in range((count + 1) // 2):
        order += [i] if 2 * i == count - 1 else [i, count - 1 - i]
    return order


def remote(src, dst, send_sem, recv_sem, peer):
    return pltpu.make_async_remote_copy(
        src_ref=src, dst_ref=dst, send_sem=send_sem, recv_sem=recv_sem, device_id=peer, device_id_type=MESH
    )


def encode(values):
    half = values.shape[0] // 2
    most = jnp.max(jnp.abs(values), axis=0, keepdims=True)
    inverse = jnp.where(most > 1e-30, CODE / most, 0.0)
    codes = (values * inverse + (MIDDLE + 0.5)).astype(jnp.int32)
    packed = codes[:half] | lax.shift_left(codes[half:], jnp.int32(16))
    return packed, most * (1.0 / CODE)


def decode(packed, unit):
    low = lax.bitwise_and(packed, jnp.int32(0xFFFF)).astype(jnp.float32)
    high = lax.shift_right_logical(packed, jnp.int32(16)).astype(jnp.float32)
    return jnp.concatenate([low - MIDDLE, high - MIDDLE], axis=0) * unit


def dot(left, right, left_dim, right_dim, precision=None):
    return lax.dot_general(
        left,
        right,
        (((left_dim,), (right_dim,)), ((), ())),
        precision=precision,
        preferred_element_type=jnp.float32,
    )


def split_terms(values):
    high = values.astype(jnp.bfloat16)
    return high, (values - high.astype(jnp.float32)).astype(jnp.bfloat16)


def whiten_start(gram, left, right):
    width = gram.shape[0]
    eye = lax.broadcasted_iota(jnp.int32, (width, width), 0) == lax.broadcasted_iota(jnp.int32, (width, width), 1)
    diagonal = jnp.where(eye, gram, 0.0)
    trace = jnp.sum(jnp.sum(diagonal, axis=1, keepdims=True), axis=0, keepdims=True)
    left[...] = gram + jnp.where(eye, 1e-05 * trace / width, 0.0)
    right[...] = jnp.where(eye, 1.0, 0.0)


def whiten_panels(start, stop, scale, out_ref, left, right):
    width = left.shape[0]
    place = lax.broadcasted_iota(jnp.int32, (8, width), 0)

    def spread(rows, step):
        return [jnp.broadcast_to(rows[:, 8 * step + i : 8 * step + i + 1], (8, width)) for i in range(8)]

    ahead = []
    for step in range(start, stop):
        here = slice(8 * step, 8 * step + 8)
        rows_left, rows_right = left[here, :], right[here, :]
        columns = ahead if ahead else spread(rows_left, step)
        inverses, tops_left, tops_right, pivots = [], [], [], []
        ahead = []
        done_right = jnp.zeros((8, width), jnp.float32)
        for i in range(8):
            inverse = lax.rsqrt(columns[i][i : i + 1, :])
            top_left, top_right = rows_left[i : i + 1, :] * inverse, rows_right[i : i + 1, :] * inverse
            done_right = jnp.where(place == i, top_right, done_right)
            factor = jnp.where(place > i, columns[i] * inverse, 0.0)
            rows_left = rows_left - factor * top_left
            rows_right = rows_right - factor * top_right
            pivot = {}
            for j in range(i + 1, 8):
                pivot[j] = columns[j][i : i + 1, :] * inverse
                columns[j] = columns[j] - factor * pivot[j]
            inverses.append(inverse)
            tops_left.append(top_left)
            tops_right.append(top_right)
            pivots.append(pivot)
        out_ref[here, :] = done_right * scale
        for block in range(step + 1, width // 8):
            there = slice(8 * block, 8 * block + 8)
            rows_left, rows_right = left[there, :], right[there, :]
            columns = spread(rows_left, step)
            if block == step + 1:
                ahead = spread(rows_left, block)
            for i in range(8):
                factor = columns[i] * inverses[i]
                if block == step + 1:
                    ahead = [ahead[j] - factor * factor[j : j + 1, :] for j in range(8)]
                rows_left = rows_left - factor * tops_left[i]
                rows_right = rows_right - factor * tops_right[i]
                for j in range(i + 1, 8):
                    columns[j] = columns[j] - factor * pivots[i][j]
            left[there, :] = rows_left
            right[there, :] = rows_right


def loop(count, body):
    lax.fori_loop(0, count, lambda i, carry: (body(i), carry)[1], 0)


def staged(count, lag, step):
    lag = min(lag, count)
    loop(lag, lambda i: step(i, True, False))
    lax.fori_loop(lag, count, lambda i, carry: (step(i, True, True), carry)[1], 0)
    lax.fori_loop(count, count + lag, lambda i, carry: (step(i, False, True), carry)[1], 0)


def two_term_loads(packed, unit, wide):
    high, low = split_terms(decode(packed, unit))
    loads = dot(jnp.concatenate([high, low], axis=1), wide, 1, 0)
    half = loads.shape[1] // 2
    return loads[:, :half] + loads[:, half:]


def write_body(
    gene_dev, gene_scale, terms, wide_ref, sums, units, basis_out, load_out, basis, loadings, basis_sem, load_sem
):
    chunks = terms.shape[0]
    width = basis.shape[1]
    wide = wide_ref[...]
    parts, members, part_rows, _ = sums.shape
    copies = []
    for k, start in enumerate(range(0, chunks, GROUP)):
        stop = min(start + GROUP, chunks)
        for i in range(start, stop):
            rows = dot(terms[i].reshape(CHUNK, 2 * width), wide, 1, 0)
            basis[i * CHUNK : (i + 1) * CHUNK, :] = rows[:, :width] + rows[:, width:]
        rows = pl.ds(start * CHUNK, (stop - start) * CHUNK)
        copies.append(pltpu.make_async_copy(basis.at[rows], basis_out.at[rows], basis_sem.at[k]))
        copies[-1].start()
    for p in range(members):
        for q in range(parts):
            start = 2 * part_rows * (p * parts + q)
            stop = min(start + 2 * part_rows, gene_dev)
            if stop > start:
                loads = two_term_loads(sums[q, p], units[q, p], wide) * gene_scale
                loadings[start:stop, :] = loads[: stop - start]
    copies.append(pltpu.make_async_copy(loadings, load_out, load_sem))
    copies[-1].start()
    for copy in copies:
        copy.wait()


def body(
    n,
    m,
    gene_dev,
    limit,
    gene_scale,
    counts_ref,
    sketch_ref,
    last_terms,
    wide_ref,
    last_sum,
    last_unit,
    counts,
    resid,
    gene_acc,
    frac,
    omega,
    part,
    near,
    codes,
    units,
    first_terms,
    product,
    gram_acc,
    gene_all,
    cell_all,
    grand_all,
    gram_all,
    gram_rows,
    gram_part,
    gram_pair,
    load_part,
    load_part_unit,
    load_all,
    load_unit,
    swap,
    swap_unit,
    first_sum,
    first_unit,
    left,
    right,
    white,
    in_sem,
    gene_sem,
    cell_sem,
    grand_sem,
    near_sem,
    code_sem,
    unit_sem,
    term_sem,
    pair_sem,
    gram_sem,
    rows_sem,
    piece_sem,
    piece_unit_sem,
    swap_sem,
    swap_unit_sem,
    all_sem,
    all_unit_sem,
):
    f32, bf16 = jnp.float32, jnp.bfloat16
    chunks, rows8, _ = counts.shape
    parts = load_all.shape[1]
    padded = resid.shape[1]
    width = left.shape[0]
    gene_rows = padded // 128
    cells_me, genes_me = lax.axis_index("cells"), lax.axis_index("genes")
    y_count = m // 2
    core, row = lax.rem(genes_me, 2), lax.div(genes_me, 2)
    partner = {"genes": row * 2 + 1 - core}
    y_peers = [{"genes": lax.rem(row + step, y_count) * 2 + core} for step in range(1, y_count)]
    beside = {"cells": lax.rem(cells_me + 1, n)}
    parity, level = lax.rem(cells_me, 2), lax.div(cells_me, 2)
    pair = {"cells": 2 * level + 1 - parity}

    def fetch(i):
        start = pl.multiple_of(i * CHUNK, CHUNK)
        return pltpu.make_async_copy(counts_ref.at[:, pl.ds(start, CHUNK)], counts.at[i], in_sem.at[i])

    loop(chunks, lambda i: fetch(i).start())
    sketch_copy = pltpu.make_async_copy(sketch_ref, omega.at[pl.ds(0, rows8)], in_sem.at[chunks])
    sketch_copy.start()
    barrier = pltpu.get_barrier_semaphore()

    def other(s):
        return {"cells": lax.rem(cells_me + lax.div(s, m), n), "genes": lax.rem(genes_me + lax.rem(s, m), m)}

    def greet(s):
        pl.semaphore_signal(barrier, inc=1, device_id=other(s + 1), device_id_type=MESH)

    loop(n * m - 1, greet)
    gene_acc[...] = jnp.zeros(gene_acc.shape, jnp.int32)
    if padded > rows8:
        omega[rows8:, :] = jnp.zeros((padded - rows8, width), bf16)
    step_rows = max(k for k in range(8, 65, 8) if rows8 % k == 0)

    def total_chunk(i):
        fetch(i).wait()

        def add(k, total):
            start = pl.ds(pl.multiple_of(k * step_rows, 8), step_rows)
            block = counts[i, start, :]
            gene_acc[start, :] += block[:, :HALF] + block[:, HALF:]
            for r in range(0, step_rows, 8):
                total = total + block[r : r + 8, :]
            return total

        total = lax.fori_loop(0, rows8 // step_rows, add, jnp.zeros((8, CHUNK), jnp.int32))
        cell_all[genes_me, i] = jnp.sum(total, axis=0, keepdims=True).astype(f32)

    with jax.named_scope("stream"):
        loop(chunks, total_chunk)
    for b in range(gene_rows):
        across = gene_acc[128 * b : 128 * (b + 1), :].astype(f32).T
        gene_row = jnp.sum(across, axis=0, keepdims=True)
        gene_all[cells_me, b] = gene_row
        grand = gene_row if b == 0 else grand + gene_row
    grand_all[cells_me * m + genes_me] = jnp.broadcast_to(jnp.sum(grand, axis=1, keepdims=True), (1, 128))
    with jax.named_scope("barrier"):
        pl.semaphore_wait(barrier, n * m - 1)

    def share(buffer, axis, me, sem):
        here = buffer.at[me]
        count = lax.axis_size(axis)
        for p in far_first(count):

            @pl.when(p != me)
            def _():
                remote(here, here, sem.at[0], sem.at[1], {axis: p}).start()

        everything = buffer.at[pl.ds(0, count - 1)]
        return remote(everything, everything, sem.at[0], sem.at[1], {axis: lax.rem(me + 1, count)})

    gene_copies = share(gene_all, "cells", cells_me, gene_sem)
    cell_copies = share(cell_all, "genes", genes_me, cell_sem)
    me = cells_me * m + genes_me

    def grand_start(s):
        here = grand_all.at[me]
        remote(here, here, grand_sem.at[0], grand_sem.at[1], other(s + 1)).start()

    loop(n * m - 1, grand_start)
    everything = grand_all.at[pl.ds(0, n * m - 1)]
    grand_copies = remote(everything, everything, grand_sem.at[0], grand_sem.at[1], other(1))
    with jax.named_scope("wait_gene"):
        gene_copies.wait_recv()
    gene_total = gene_all[0]
    for s in range(1, n):
        gene_total = gene_total + gene_all[s]
    with jax.named_scope("wait_grand"):
        grand_copies.wait_recv()
    grand = jnp.sum(grand_all[...], axis=0)
    for b in range(gene_rows):
        share_row = jnp.where(gene_total[b] > 0.0, gene_total[b] / grand, 1.0)
        frac[128 * b : 128 * (b + 1), :] = jnp.broadcast_to(share_row, (128, 128)).T
    with jax.named_scope("wait_cell"):
        cell_copies.wait_recv()

    low_limit, high_limit = jnp.asarray(-limit, bf16), jnp.asarray(limit, bf16)

    def residual(i):
        cell_total = cell_all[0, i]
        for s in range(1, m):
            cell_total = cell_total + cell_all[s, i]
        sums = None
        for start in range(0, padded, DEPTH):
            stop = min(start + DEPTH, padded)
            blocks = []
            for k in range(start, min(stop, rows8), BLOCK):
                real = min(k + BLOCK, stop, rows8) - k
                share_of = frac[k : k + real, :]
                expected = jnp.concatenate([share_of, share_of], axis=1) * cell_total
                scaled = (counts[i, k : k + real, :].astype(f32) - expected) * lax.rsqrt(
                    expected + 0.01 * expected * expected
                )
                blocks.append(scaled)
            if stop > rows8:
                blocks.append(jnp.zeros((stop - max(start, rows8), CHUNK), f32))
            values = jnp.clip(jnp.concatenate(blocks, axis=0).astype(bf16), low_limit, high_limit)
            resid[i, start:stop, :] = values
            term = dot(values, omega[start:stop, :], 0, 0)
            sums = term if sums is None else sums + term
        return sums

    sketch_copy.wait()
    for sweep in range(ITERS):
        last = sweep == ITERS - 1
        terms = last_terms if last else first_terms
        load_sum, load_sum_unit = (last_sum, last_unit) if last else (first_sum, first_unit)

        def near_copy(i):
            return remote(part.at[i, 1 - core], near.at[sweep, i], near_sem.at[chunks], near_sem.at[i], partner)

        def code_start(i):
            for peer in y_peers:
                for buffer, sem in ((codes, code_sem), (units, unit_sem)):
                    here = buffer.at[sweep, row, i]
                    remote(here, here, sem.at[chunks], sem.at[i], peer).start()

        def code_wait(i):
            for buffer, sem in ((codes, code_sem), (units, unit_sem)):
                here = buffer.at[sweep, pl.ds(0, y_count - 1), i]
                remote(here, here, sem.at[chunks], sem.at[i], y_peers[0]).wait_recv()

        def term_copy(i):
            here = terms.at[i, core]
            return remote(here, here, term_sem.at[chunks], term_sem.at[i], partner)

        def first(i, sketch, code):
            j = i - NEAR_LAG
            if code:
                near_copy(j).wait_recv()
                packed, unit = encode(part[j, core] + near[sweep, j])
                codes[sweep, row, j] = packed
                units[sweep, row, j] = unit
            if sketch:
                rows = residual(i) if sweep == 0 else dot(resid[i], omega[...], 0, 0)
                part[i, 0] = rows[:HALF]
                part[i, 1] = rows[HALF:]
                near_copy(i).start()
            if code:
                code_start(j)

        def second(i, decoding, multiply):
            j = i - BASIS_LAG
            if decoding:
                code_wait(i)
            if multiply:
                term_copy(j).wait_recv()
                both = terms[j].reshape(CHUNK, 2 * width)
                gram_acc[...] += dot(both, both, 0, 0)
                product[...] += dot(resid[j], both, 1, 0)
            if decoding:
                total = decode(codes[sweep, 0, i], units[sweep, 0, i])
                for s in range(1, y_count):
                    total = total + decode(codes[sweep, s, i], units[sweep, s, i])
                high, low = split_terms(total)
                terms[i, core] = jnp.concatenate([high, low], axis=1)
                term_copy(i).start()

        with jax.named_scope(f"first{sweep}"):
            staged(chunks, NEAR_LAG, first)
        product[...] = jnp.zeros(product.shape, f32)
        gram_acc[...] = jnp.zeros(gram_acc.shape, f32)
        with jax.named_scope(f"second{sweep}"):
            staged(chunks, BASIS_LAG, second)

        gram = gram_acc[:width, :width] + gram_acc[:width, width:] + (gram_acc[width:, :width] + gram_acc[width:, width:])
        gram_part[...] = gram.reshape(gram_part.shape)
        pair_copy = remote(
            gram_part.at[genes_me, 1 - parity], gram_pair.at[sweep], pair_sem.at[sweep, 0], pair_sem.at[sweep, 1], pair
        )
        pair_copy.start()
        members = n // 2
        piece = padded // members
        part_rows = piece // 2 // parts
        side, member = lax.div(cells_me, members), lax.rem(cells_me, members)
        across = {"cells": (1 - side) * members + member}
        stage_sems = ((load_all, piece_sem), (load_unit, piece_unit_sem))

        def scatter(q):
            for p in range(members):
                start = p * piece + q * 2 * part_rows
                rows = product[start : start + 2 * part_rows, :]
                packed, unit = encode(rows[:, :width] + rows[:, width:])
                load_part[sweep, q, p] = packed
                load_part_unit[sweep, q, p] = unit

                @pl.when(p != member)
                def _():
                    for src, (dst, sem) in zip((load_part, load_part_unit), stage_sems):
                        sems = sem.at[q, 0], sem.at[q, 1]
                        remote(
                            src.at[sweep, q, p], dst.at[sweep, q, member], *sems, {"cells": side * members + p}
                        ).start()

            load_all[sweep, q, member] = load_part[sweep, q, member]
            load_unit[sweep, q, member] = load_part_unit[sweep, q, member]

        def most_of(buffer, sem):
            most = buffer.at[pl.ds(0, members - 1)]
            return remote(most, most, sem.at[0], sem.at[1], across)

        piece_copies = [
            most_of(dst.at[sweep, q], sem.at[q]) for q in range(parts) for dst, sem in stage_sems
        ]

        def swap_copies(q):
            return [
                remote(buffer.at[sweep, q, side], buffer.at[sweep, q, side], sem.at[sweep, q, 0], sem.at[sweep, q, 1], across)
                for buffer, sem in ((swap, swap_sem), (swap_unit, swap_unit_sem))
            ]

        def cross(q):
            with jax.named_scope(f"wait_piece{q}{sweep}"):
                piece_copies[2 * q].wait_recv()
                piece_copies[2 * q + 1].wait_recv()
            total = decode(load_all[sweep, q, 0], load_unit[sweep, q, 0])
            for s in range(1, members):
                total = total + decode(load_all[sweep, q, s], load_unit[sweep, q, s])
            packed, unit = encode(total)
            swap[sweep, q, side] = packed
            swap_unit[sweep, q, side] = unit
            for copy in swap_copies(q):
                copy.start()

        all_copies = []

        def gather(q):
            with jax.named_scope(f"wait_swap{q}{sweep}"):
                for copy in swap_copies(q):
                    copy.wait_recv()
            total = decode(swap[sweep, q, 0], swap_unit[sweep, q, 0])
            total = total + decode(swap[sweep, q, 1], swap_unit[sweep, q, 1])
            packed, unit = encode(total)
            load_sum[q, member] = packed
            load_sum_unit[q, member] = unit
            for buffer, sem in ((load_sum, all_sem), (load_sum_unit, all_unit_sem)):
                here = buffer.at[q, member]
                for p in range(members):

                    @pl.when(p != member)
                    def _():
                        remote(here, here, sem.at[q, 0], sem.at[q, 1], {"cells": side * members + p}).start()

                all_copies.append(most_of(buffer.at[q], sem.at[q]))

        def level_sum():
            pair_copy.wait()
            gram_all[sweep, level] = gram_part[genes_me, parity] + gram_pair[sweep]
            for p in far_first(n // 2):
                here = gram_all.at[sweep, level]

                @pl.when(p != level)
                def _():
                    remote(here, here, gram_sem.at[sweep, 0], gram_sem.at[sweep, 1], {"cells": 2 * p + parity}).start()

            everything = gram_all.at[sweep, pl.ds(0, n // 2 - 1)]
            gram_copies = remote(everything, everything, gram_sem.at[sweep, 0], gram_sem.at[sweep, 1], beside)
            return gram_copies

        for q in range(parts):
            scatter(q)
        gram_copies = level_sum()
        for q in range(parts):
            cross(q)
        with jax.named_scope(f"wait_gram{sweep}"):
            gram_copies.wait_recv()
        total = gram_all[sweep, 0]
        for s in range(1, n // 2):
            total = total + gram_all[sweep, s]
        mine = 2 * genes_me + parity
        gram_rows[sweep, mine] = total
        here = gram_rows.at[sweep, mine]
        for step in range(1, 2 * m):
            peer = {"genes": lax.rem(genes_me + step // 2, m)}
            if step % 2:
                peer["cells"] = pair["cells"]
            remote(here, here, rows_sem.at[sweep, 0], rows_sem.at[sweep, 1], peer).start()
        everything = gram_rows.at[sweep, pl.ds(0, 2 * m - 1)]
        rows_copies = remote(everything, everything, rows_sem.at[sweep, 0], rows_sem.at[sweep, 1], beside)
        for q in range(parts):
            gather(q)
        with jax.named_scope(f"wait_rows{sweep}"):
            rows_copies.wait_recv()
        scale = math.sqrt(chunks * CHUNK * n)
        with jax.named_scope(f"whiten{sweep}"):
            whiten_start(gram_rows[sweep].reshape(width, width), left, right)
            whiten_panels(0, width // 8, scale, white, left, right)
        high, low = split_terms(white[...].T)
        wide = jnp.concatenate([high, low], axis=1)
        wide = jnp.concatenate([wide, wide], axis=0)
        if last:
            wide_ref[...] = wide
        with jax.named_scope(f"wait_all{sweep}"):
            for copies in all_copies:
                copies.wait_recv()
        if not last:
            for p in range(members):
                for q in range(parts):
                    loads = two_term_loads(load_sum[q, p], load_sum_unit[q, p], wide)
                    start = piece * p + 2 * part_rows * q
                    omega[start : start + 2 * part_rows, :] = (loads * gene_scale).astype(bf16)
        for copies in [gram_copies, rows_copies] + all_copies + piece_copies + swap_copies(0) + swap_copies(parts - 1)[: 2 * (parts - 1)]:
            copies.wait_send()
        near_all, term_all = near.at[sweep], terms.at[pl.ds(0, chunks), core]
        remote(near_all, near_all, near_sem.at[chunks], near_sem.at[0], partner).wait_send()
        remote(term_all, term_all, term_sem.at[chunks], term_sem.at[0], partner).wait_send()
        for buffer, sem in ((codes, code_sem), (units, unit_sem)):
            here = buffer.at[sweep, pl.ds(0, y_count - 1)]
            remote(here, here, sem.at[chunks], sem.at[0], y_peers[0]).wait_send()
    for copies in (gene_copies, cell_copies, grand_copies):
        copies.wait_send()


def shards(counts, sketch):
    cell_dev, gene_dev = counts.shape
    n, m = lax.axis_size("cells"), lax.axis_size("genes")
    width = sketch.shape[1]
    rows8 = -(-gene_dev // 8) * 8
    unit = max(16 * n, 128)
    padded = -(-gene_dev // unit) * unit
    chunks = cell_dev // CHUNK
    strip = width // (2 * m)
    assert chunks * CHUNK == cell_dev and m % 2 == 0 and n % 2 == 0 and strip % 8 == 0
    table = counts.T
    if rows8 > gene_dev:
        table = jnp.pad(table, ((0, rows8 - gene_dev), (0, 0)))
        sketch = jnp.pad(sketch, ((0, rows8 - gene_dev), (0, 0)))
    cell_count = float(cell_dev * n)
    gene_scale = math.sqrt(float(gene_dev * m)) / cell_count
    f32, bf16, i32 = jnp.float32, jnp.bfloat16, jnp.int32
    y_count = m // 2
    members = n // 2
    piece = padded // members
    parts = 2 if piece % 32 == 0 else 1
    part_rows = piece // 2 // parts
    vmem = pltpu.VMEM
    dma = pltpu.SemaphoreType.DMA
    scratch = [
        vmem((chunks, rows8, CHUNK), i32),
        vmem((chunks, padded, CHUNK), bf16),
        vmem((padded, 128), i32),
        vmem((padded, 128), f32),
        vmem((padded, width), bf16),
        vmem((chunks, 2, HALF, width), f32),
        vmem((ITERS, chunks, HALF, width), f32),
        vmem((ITERS, y_count, chunks, HALF // 2, width), i32),
        vmem((ITERS, y_count, chunks, 1, width), f32),
        vmem((chunks, 2, HALF, 2 * width), bf16),
        vmem((padded, 2 * width), f32),
        vmem((2 * width, 2 * width), f32),
        vmem((n, padded // 128, 1, 128), f32),
        vmem((m, chunks, 1, CHUNK), f32),
        vmem((n * m, 1, 128), f32),
        vmem((ITERS, n // 2, strip, width), f32),
        vmem((ITERS, 2 * m, strip, width), f32),
        vmem((m, 2, strip, width), f32),
        vmem((ITERS, strip, width), f32),
        vmem((ITERS, parts, members, part_rows, width), i32),
        vmem((ITERS, parts, members, 1, width), f32),
        vmem((ITERS, parts, members, part_rows, width), i32),
        vmem((ITERS, parts, members, 1, width), f32),
        vmem((ITERS, parts, 2, part_rows, width), i32),
        vmem((ITERS, parts, 2, 1, width), f32),
        vmem((parts, members, part_rows, width), i32),
        vmem((parts, members, 1, width), f32),
        vmem((width, width), f32),
        vmem((width, width), f32),
        vmem((width, width), f32),
        dma((chunks + 1,)),
        dma((2,)),
        dma((2,)),
        dma((2,)),
        dma((chunks + 1,)),
        dma((chunks + 1,)),
        dma((chunks + 1,)),
        dma((chunks + 1,)),
        dma((ITERS, 2)),
        dma((ITERS, 2)),
        dma((ITERS, 2)),
        dma((parts, 2)),
        dma((parts, 2)),
        dma((ITERS, parts, 2)),
        dma((ITERS, parts, 2)),
        dma((parts, 2)),
        dma((parts, 2)),
    ]
    handed = [
        jax.ShapeDtypeStruct((chunks, 2, HALF, 2 * width), bf16),
        jax.ShapeDtypeStruct((2 * width, 2 * width), bf16),
        jax.ShapeDtypeStruct((parts, members, part_rows, width), i32),
        jax.ShapeDtypeStruct((parts, members, 1, width), f32),
    ]
    handed = pl.pallas_call(
        functools.partial(body, n, m, gene_dev, math.sqrt(cell_count), gene_scale),
        out_shape=handed,
        in_specs=[pl.BlockSpec(memory_space=pltpu.HBM)] * 2,
        out_specs=[pl.BlockSpec(memory_space=pltpu.VMEM)] * 4,
        scratch_shapes=scratch,
        compiler_params=pltpu.CompilerParams(
            collective_id=0, has_side_effects=True, vmem_limit_bytes=48 * 1024 * 1024
        ),
    )(table, sketch)
    return pl.pallas_call(
        functools.partial(write_body, gene_dev, gene_scale),
        out_shape=[jax.ShapeDtypeStruct((cell_dev, width), f32), jax.ShapeDtypeStruct((gene_dev, width), f32)],
        in_specs=[pl.BlockSpec(memory_space=pltpu.VMEM)] * 4,
        out_specs=[pl.BlockSpec(memory_space=pltpu.HBM)] * 2,
        scratch_shapes=[
            vmem((cell_dev, width), f32),
            vmem((gene_dev, width), f32),
            dma((-(-chunks // GROUP),)),
            dma(()),
        ],
        compiler_params=pltpu.CompilerParams(vmem_limit_bytes=16 * 1024 * 1024),
    )(*handed)


def solution(mesh):
    return jax.shard_map(
        shards,
        mesh=mesh,
        in_specs=(P("cells", "genes"), P("genes", None)),
        out_specs=(P("cells", None), P("genes", None)),
        check_vma=False,
    )
```
